32 devices in a mesh: grp: 2 (over x), row: 16 (over z, y, core).
Axes of the slice: x: 2, y: 2, z: 4, core: 2. Of those that a mesh axis runs over, the one named last changes fastest.
Arguments:
- slc: bfloat16 [2, 300, 64, 256], P(None, None, ('grp', 'row')), parts along dimension 2, may hold values from -8 to 8
- mask: int32 [25, 64, 256], P(None, ('grp', 'row')), parts along dimension 1, may hold values 0 or 1
- ref_index: int32 [2], P('grp'), parts along dimension 0, may hold values from 0 to 8191
Outputs:
- linked: float32 [2, 300, 64, 256], P(None, None, ('grp', 'row')), parts along dimension 2
The draws below stay inside these ranges and needn't reach their ends.
There are 2 independent parts, one for each index of `grp`. The reference program is written for one: setup_inputs(seed, part) draws one part's arguments, and reference() takes and returns one part's arrays. A program takes and returns all parts, laid end to end along the dimension named above; each array names one. Nothing has to cross between parts.
All inputs are finite; a program needn't handle non-finite values. No bound on the sum of `mask` on one device may be relied on, other than what follows from the above.
Results may differ from the reference program's by a relative error of at most 0.0046.
Values may be sent and summed in bfloat16 or wider, within the bound.
A program may use at most 64 MiB of HBM per device.

```python
import math
import jax
import jax.numpy as jnp
from jax import lax

NDATE = 300
NC = 256
HALF = 2
ITERS = 2
OFFS = 25
NR = 32


def draw_slc(key, part):
    first, second, third = jax.random.split(key, 3)
    noise = jax.random.normal(first, (2, NDATE, NR, NC), jnp.float32)
    logamp = jax.random.uniform(second, (1, NDATE, NR, 1), jnp.float32, math.log(0.5), math.log(2.0))
    field = noise
    return jnp.clip(jnp.exp(logamp) * field, -8.0, 8.0).astype(jnp.bfloat16)


def with_ends(drawn, stream_key, smallest, high):
    longest = drawn.shape.index(max(drawn.shape))
    spots = []
    for shift in (0, 1):
        where = [jax.random.randint(jax.random.fold_in(stream_key, axis), (), 0, length) for axis, length in enumerate(drawn.shape)]
        where[longest] = (where[longest] + shift) % drawn.shape[longest]
        spots.append(tuple(where))
    return drawn.at[spots[0]].set(smallest).at[spots[1]].set(high)


def setup_inputs(seed: int = 0, part: int = 0) -> dict:
    keys = jax.random.split(jax.random.key(seed), 4)
    part_splits = jax.random.split(jax.random.fold_in(keys[3], part), 4)
    return {
        "slc": draw_slc(jax.random.fold_in(jax.random.fold_in(keys[3], part), 71), part),
        "mask": with_ends((jax.random.randint(part_splits[1], (OFFS, NR, NC), 0, 2) < 1).astype(jnp.int32), jax.random.fold_in(part_splits[1], 1), 0, 1),
        "ref_index": jax.random.randint(part_splits[2], (1,), 0, NR * NC).astype(jnp.int32),
    }


def link_pixels(extended, mask, total_rows):
    rows = extended.shape[2] - 2 * HALF
    cols = extended.shape[3]
    padded = jnp.pad(extended, ((0, 0), (0, 0), (0, 0), (HALF, HALF)))
    row_ids = jnp.arange(rows)[:, None]
    col_ids = jnp.arange(cols)[None, :]
    width = 2 * HALF + 1
    weights = []
    count = jnp.zeros((rows, cols), jnp.float32)
    for row_shift in range(-HALF, HALF + 1):
        for col_shift in range(-HALF, HALF + 1):
            offset = (row_shift + HALF) * width + col_shift + HALF
            inside = (row_ids + row_shift >= 0) & (row_ids + row_shift < total_rows)
            inside = inside & (col_ids + col_shift >= 0) & (col_ids + col_shift < cols)
            if row_shift == 0 and col_shift == 0:
                chosen = inside
            else:
                chosen = inside & (mask[offset] == 1)
            weight = chosen.astype(jnp.float32)
            weights.append(weight)
            count = count + weight
    inverse = 1.0 / count
    vector = padded[:, :, HALF:HALF + rows, HALF:HALF + cols].astype(jnp.float32)
    for step in range(ITERS):
        total_real = jnp.zeros((NDATE, rows, cols), jnp.float32)
        total_imag = jnp.zeros((NDATE, rows, cols), jnp.float32)
        for row_shift in range(-HALF, HALF + 1):
            for col_shift in range(-HALF, HALF + 1):
                offset = (row_shift + HALF) * width + col_shift + HALF
                piece = padded[:, :, HALF + row_shift:HALF + row_shift + rows, HALF + col_shift:HALF + col_shift + cols].astype(jnp.float32)
                proj_real = lax.optimization_barrier(jnp.sum(piece[0] * vector[0] + piece[1] * vector[1], axis=0)) / NDATE
                proj_imag = lax.optimization_barrier(jnp.sum(piece[0] * vector[1] - piece[1] * vector[0], axis=0)) / NDATE
                coef_real = weights[offset] * inverse * proj_real
                coef_imag = weights[offset] * inverse * proj_imag
                total_real = total_real + coef_real * piece[0] - coef_imag * piece[1]
                total_imag = total_imag + coef_real * piece[1] + coef_imag * piece[0]
        factor = lax.rsqrt(lax.optimization_barrier(jnp.mean(total_real * total_real + total_imag * total_imag, axis=0)) + 0.001)
        vector = jnp.stack([total_real * factor, total_imag * factor])
    return vector

def reference(slc, mask, ref_index):
    row_count = slc.shape[2]
    col_count = slc.shape[3]
    data = slc.astype(jnp.float32)
    power = lax.optimization_barrier(jnp.sum(data[0] * data[0] + data[1] * data[1], axis=(1, 2)))
    gains = lax.rsqrt(power / (row_count * col_count) + 0.1)
    scaled = (data * gains[:, None, None]).astype(jnp.bfloat16)
    extended = jnp.pad(scaled, ((0, 0), (0, 0), (HALF, HALF), (0, 0)))
    vector = link_pixels(extended, mask, row_count)
    target = ref_index[0].astype(jnp.int32)
    row_target = (target // col_count).astype(jnp.int32)
    col_target = (target % col_count).astype(jnp.int32)
    zero = jnp.zeros((), jnp.int32)
    picked = lax.dynamic_slice(vector, (zero, zero, row_target, col_target), (2, NDATE, 1, 1))
    real_ref = picked[0]
    imag_ref = picked[1]
    out_real = vector[0] * real_ref + vector[1] * imag_ref
    out_imag = vector[1] * real_ref - vector[0] * imag_ref
    return jnp.stack([out_real, out_imag])
```

```python
import jax
import jax.numpy as jnp
from jax import lax
from jax.experimental import pallas as pl
from jax.experimental.pallas import tpu as pltpu
from jax.sharding import PartitionSpec as P

HALF = 2
ITERS = 2
WIDTH = 2 * HALF + 1
LANE = 128
SUB = 16
MESH = pl.DeviceIdType.MESH


def round_up(value, unit):
    return (value + unit - 1) // unit * unit


def kernel(
    n, ndate, x_hbm, mask_ref, index_ref, out_ref,
    raw, wide, scene, turned, chosen, weight, pairs, coef, total, vectors, gains, column, powers, refs,
    load_sem, far_sem, near_sem, power_sem, ref_sem,
):
    _, rows, cols = mask_ref.shape
    span, blocks, depth, _ = scene.shape
    half = depth // 2
    long_depth = refs.shape[2]
    long_dates = powers.shape[2]
    total_rows = rows * n
    stride = blocks * rows
    me = lax.axis_index("row")
    odd = lax.rem(me, 2)
    near = me + 1 - 2 * odd
    far = me - 1 + 2 * odd
    has_near = near < n
    has_far = (far >= 0) & (far < n)
    first_row = me * rows

    def peer(k):
        return lax.rem(me + k, n)

    def place(q):
        return q + odd * (rows - 1 - 2 * q)

    load = pltpu.make_async_copy(x_hbm, raw, load_sem)
    load.start()
    barrier = pltpu.get_barrier_semaphore()

    @pl.loop(1, n)
    def _(k):
        pl.semaphore_signal(barrier, inc=1, device_id={"row": peer(k)}, device_id_type=MESH)

    row_ids = first_row + lax.broadcasted_iota(jnp.int32, (rows, cols), 0)
    col_ids = lax.broadcasted_iota(jnp.int32, (rows, cols), 1)
    count = jnp.zeros((rows, cols), jnp.float32)
    for a in range(WIDTH):
        step = a + odd * (WIDTH - 1 - 2 * a)
        for b in range(WIDTH):
            there = row_ids + (step - HALF)
            inside = (there >= 0) & (there < total_rows)
            inside = inside & (col_ids + (b - HALF) >= 0) & (col_ids + (b - HALF) < cols)
            if (a, b) != (HALF, HALF):
                inside = inside & (mask_ref[step * WIDTH + b] == 1)
            one = inside.astype(jnp.float32)
            chosen[a * WIDTH + b] = one
            count = count + one
    inverse = 1.0 / (count * ndate)
    for o in range(WIDTH * WIDTH):
        chosen[o] = chosen[o] * inverse

    def window(block):
        return max(0, block * LANE - SUB), min(cols, (block + 1) * LANE + SUB)

    coef[...] = jnp.zeros_like(coef)
    for block in range(blocks):
        begin, end = window(block)
        shape = (end - begin, LANE)
        shift = begin - block * LANE
        shift = shift + lax.broadcasted_iota(jnp.int32, shape, 0) - lax.broadcasted_iota(jnp.int32, shape, 1)
        for q in range(rows):
            for a in range(WIDTH):
                band = jnp.zeros(shape, jnp.float32)
                for b in range(WIDTH):
                    lanes = slice(block * LANE, (block + 1) * LANE)
                    line = chosen[a * WIDTH + b, q:q + 1, lanes]
                    line = jnp.where(odd == 1, chosen[a * WIDTH + b, rows - 1 - q:rows - q, lanes], line)
                    band = jnp.where(shift == b - HALF, line, band)
                weight[block, q, a, 0:end - begin, :] = band

    column[...] = jnp.zeros_like(column)

    load.wait()
    wide[0:raw.shape[0], :] = raw[...].astype(jnp.float32)
    sums = jnp.zeros((half, LANE), jnp.float32)
    dates = lax.broadcasted_iota(jnp.int32, (half, LANE), 0)
    for q in range(rows):
        for part in range(2):
            for block in range(blocks):
                start = part * ndate * stride + block * rows + place(q)
                piece = wide[pl.ds(start, half, stride=stride), :]
                piece = jnp.where(dates < ndate, piece, 0.0)
                scene[HALF + q, block, part * half:(part + 1) * half, :] = piece.astype(jnp.bfloat16)
                sums = sums + piece * piece
    column[0:half, :] = sums
    powers[me] = jnp.sum(column[0:long_dates, :].T, axis=0, keepdims=True)

    pl.semaphore_wait(barrier, n - 1)

    def exchange(buffer, sems):
        def copy(k, slot):
            return pltpu.make_async_remote_copy(
                src_ref=buffer.at[slot], dst_ref=buffer.at[slot],
                send_sem=sems.at[0, k], recv_sem=sems.at[1, slot],
                device_id={"row": peer(k)}, device_id_type=MESH,
            )

        def start():
            @pl.loop(1, n)
            def _(k):
                copy(k, me).start()

        def finish():
            @pl.loop(1, n)
            def _(k):
                copy(k, peer(k)).wait_recv()

            @pl.loop(1, n)
            def _(k):
                copy(k, me).wait_send()

        return start, finish

    start_power, finish_power = exchange(powers, power_sem)
    start_ref, finish_ref = exchange(refs, ref_sem)
    start_power()

    far_id = jnp.clip(far, 0, n - 1)
    near_id = jnp.clip(near, 0, n - 1)

    def far_copy(t):
        return pltpu.make_async_remote_copy(
            src_ref=scene.at[HALF + t], dst_ref=scene.at[HALF - 1 - t],
            send_sem=far_sem.at[0, t], recv_sem=far_sem.at[1, t],
            device_id={"row": far_id}, device_id_type=MESH,
        )

    def near_copy(t):
        return pltpu.make_async_remote_copy(
            src_ref=scene.at[HALF + rows - 1 - t], dst_ref=scene.at[HALF + rows + t],
            send_sem=near_sem.at[0, t], recv_sem=near_sem.at[1, t],
            device_id={"row": near_id}, device_id_type=MESH,
        )

    for t in range(HALF):
        pl.when(has_far)(far_copy(t).start)
    for t in range(HALF):
        pl.when(has_near)(near_copy(t).start)

    @pl.when(jnp.logical_not(has_far))
    def _():
        scene[0:HALF] = jnp.zeros((HALF, blocks, depth, LANE), scene.dtype)

    @pl.when(jnp.logical_not(has_near))
    def _():
        scene[HALF + rows:span] = jnp.zeros((HALF, blocks, depth, LANE), scene.dtype)

    def turn(slot):
        for block in range(blocks):
            tall = jnp.concatenate(
                [scene[slot, block], jnp.zeros((long_depth - depth, LANE), scene.dtype)], axis=0
            )
            turned[slot, block * LANE:(block + 1) * LANE, :] = tall.T

    for q in range(rows):
        turn(HALF + q)

    finish_power()
    power = jnp.sum(powers[...], axis=0)
    gain_row = lax.rsqrt(power * (1.0 / (total_rows * cols)) + 0.1)
    gains[...] = jnp.broadcast_to(gain_row, (LANE, long_dates)).T[0:half, :]

    def set_pair(q, block, real, imag):
        pairs[q, block, 0:half, 0:LANE] = real
        pairs[q, block, 0:half, LANE:2 * LANE] = imag
        pairs[q, block, half:depth, 0:LANE] = imag
        pairs[q, block, half:depth, LANE:2 * LANE] = -real

    for q in range(rows):
        for block in range(blocks):
            square = gains[...] * gains[...]
            tile = scene[HALF + q, block].astype(jnp.float32)
            set_pair(
                q, block, (tile[0:half] * square).astype(jnp.bfloat16), (tile[half:depth] * square).astype(jnp.bfloat16)
            )

    def project(q, block, slot):
        a = slot - q
        begin, end = window(block)
        proj = jnp.dot(turned[slot, begin:end, 0:depth], pairs[q, block], preferred_element_type=jnp.float32)
        band = weight[block, q, a, 0:end - begin, :]
        both = jnp.concatenate([band, band], axis=1)
        coef[q, block, a * cols + begin:a * cols + end, :] = (proj * both).astype(jnp.bfloat16)

    def update(q, block, slots):
        left = jnp.concatenate([scene[s, b] for s in slots for b in range(blocks)], axis=1)
        right = coef[q, block, (slots[0] - q) * cols:(slots[-1] + 1 - q) * cols, :]
        return jnp.dot(left, right, preferred_element_type=jnp.float32)

    def normalize(product):
        gain = gains[...]
        top, bottom = product[0:half], product[half:depth]
        real = (top[:, 0:LANE] - bottom[:, LANE:2 * LANE]) * gain
        imag = (top[:, LANE:2 * LANE] + bottom[:, 0:LANE]) * gain
        energy = jnp.sum(real * real + imag * imag, axis=0, keepdims=True)
        factor = lax.rsqrt(energy * (1.0 / ndate) + 0.001)
        return real * factor, imag * factor

    def rest(q, block, product):
        real, imag = normalize(product)
        for _ in range(1, ITERS):
            gain = gains[...]
            set_pair(q, block, (real * gain).astype(jnp.bfloat16), (imag * gain).astype(jnp.bfloat16))
            for slot in range(q, q + WIDTH):
                project(q, block, slot)
            real, imag = normalize(update(q, block, list(range(q, q + WIDTH))))
        vectors[q, block, 0:half, :] = real
        vectors[q, block, half:depth, :] = imag

    def seen(q, slots):
        return [s for s in slots if q <= s < q + WIDTH]

    for q in range(rows):
        for block in range(blocks):
            for slot in seen(q, range(HALF, HALF + rows)):
                project(q, block, slot)
    for t in range(HALF):
        pl.when(has_near)(near_copy(t).wait_recv)
        turn(HALF + rows + t)
    for q in range(rows):
        for block in range(blocks):
            for slot in seen(q, range(HALF + rows, span)):
                project(q, block, slot)

    def whole(q, block):
        rest(q, block, update(q, block, list(range(q, q + WIDTH))))

    for q in range(HALF, rows):
        for block in range(blocks):
            whole(q, block)
    for t in range(HALF):
        slot = HALF - 1 - t
        pl.when(has_far)(far_copy(t).wait_recv)
        turn(slot)
        for q in range(min(slot, rows - 1), -1, -1):
            for block in range(blocks):
                project(q, block, slot)
        for block in range(blocks):
            if slot > 0:
                if slot < rows:
                    whole(slot, block)
                if slot == 1:
                    total[0, block] = update(0, block, list(range(1, WIDTH)))
            else:
                rest(0, block, total[0, block] + update(0, block, [0]))

    target = index_ref[0]
    picked = jnp.zeros((depth, LANE), jnp.float32)
    for q in range(rows):
        for block in range(blocks):
            spot = (first_row + place(q)) * cols + block * LANE + lax.broadcasted_iota(jnp.int32, (1, LANE), 1)
            picked = picked + jnp.where(spot == target, vectors[q, block], 0.0)
    column[...] = jnp.zeros_like(column)
    column[0:depth, :] = picked
    refs[me] = jnp.sum(column[...].T, axis=0, keepdims=True)
    start_ref()
    finish_ref()
    refvec = jnp.sum(refs[...], axis=0)
    refvec = jnp.broadcast_to(refvec, (LANE, long_depth)).T
    ref_real = refvec[0:half]
    ref_imag = refvec[half:depth]
    for q in range(rows):
        for block in range(blocks):
            real = vectors[q, block, 0:half, :]
            imag = vectors[q, block, half:depth, :]
            start = block * rows + place(q)
            out_ref[pl.ds(start, ndate, stride=stride), :] = (real * ref_real + imag * ref_imag)[0:ndate]
            start = start + ndate * stride
            out_ref[pl.ds(start, ndate, stride=stride), :] = (imag * ref_real - real * ref_imag)[0:ndate]

    for t in range(HALF):
        pl.when(has_far)(far_copy(t).wait_send)
        pl.when(has_near)(near_copy(t).wait_send)


def per_device(slc, mask, ref_index):
    parts, ndate, rows, cols = slc.shape
    n = lax.axis_size("row")
    half = round_up(ndate, SUB)
    depth = 2 * half
    long_dates = round_up(half, LANE)
    long_depth = round_up(depth, LANE)
    blocks = cols // LANE
    span = rows + 2 * HALF
    lines = parts * ndate * blocks * rows
    x = slc.reshape(parts, ndate, rows, blocks, LANE).transpose(0, 1, 3, 2, 4).reshape(lines, LANE)
    vmem = pl.BlockSpec(memory_space=pltpu.VMEM)

    def body(*refs):
        kernel(n, ndate, *refs)

    out = pl.pallas_call(
        body,
        out_shape=jax.ShapeDtypeStruct((lines, LANE), jnp.float32),
        in_specs=[pl.BlockSpec(memory_space=pl.ANY), vmem, pl.BlockSpec(memory_space=pltpu.SMEM)],
        out_specs=vmem,
        scratch_shapes=[
            pltpu.VMEM((lines, LANE), jnp.bfloat16),
            pltpu.VMEM((lines + (half - ndate) * blocks * rows, LANE), jnp.float32),
            pltpu.VMEM((span, blocks, depth, LANE), jnp.bfloat16),
            pltpu.VMEM((span, cols, long_depth), jnp.bfloat16),
            pltpu.VMEM((WIDTH * WIDTH, rows, cols), jnp.float32),
            pltpu.VMEM((blocks, rows, WIDTH, LANE + 2 * SUB, LANE), jnp.float32),
            pltpu.VMEM((rows, blocks, depth, 2 * LANE), jnp.bfloat16),
            pltpu.VMEM((rows, blocks, WIDTH * cols, 2 * LANE), jnp.bfloat16),
            pltpu.VMEM((rows, blocks, depth, 2 * LANE), jnp.float32),
            pltpu.VMEM((rows, blocks, depth, LANE), jnp.float32),
            pltpu.VMEM((half, LANE), jnp.float32),
            pltpu.VMEM((long_depth, LANE), jnp.float32),
            pltpu.VMEM((n, 1, long_dates), jnp.float32),
            pltpu.VMEM((n, 1, long_depth), jnp.float32),
            pltpu.SemaphoreType.DMA,
            pltpu.SemaphoreType.DMA((2, HALF)),
            pltpu.SemaphoreType.DMA((2, HALF)),
            pltpu.SemaphoreType.DMA((2, n)),
            pltpu.SemaphoreType.DMA((2, n)),
        ],
        compiler_params=pltpu.CompilerParams(collective_id=0, has_side_effects=True),
        name="link",
    )(x, mask, ref_index)
    out = out.reshape(parts, ndate, blocks, rows, LANE).transpose(0, 1, 3, 2, 4)
    return out.reshape(parts, ndate, rows, cols)


def solution(mesh):
    placed = (P(None, None, ("grp", "row"), None), P(None, ("grp", "row"), None), P("grp"))
    return jax.shard_map(
        per_device,
        mesh=mesh,
        in_specs=placed,
        out_specs=P(None, None, ("grp", "row"), None),
        check_vma=False,
    )
```

```python
import jax
import jax.numpy as jnp
from jax import lax
from jax.experimental import pallas as pl
from jax.experimental.pallas import tpu as pltpu
from jax.sharding import PartitionSpec as P

HALF = 2
ITERS = 2
WIDTH = 2 * HALF + 1
LANE = 128
SUB = 16
VMEM_LIMIT = 32000000
MESH = pl.DeviceIdType.MESH


def round_up(value, unit):
    return (value + unit - 1) // unit * unit


def kernel(
    n, ndate, x_hbm, mask_hbm, index_ref, out_ref,
    raw, mask_ref, wide, scene, turned, chosen, picks, weight, pairs, coef, total, vectors, gains, long_gain, column, powers, refs,
    load_sem, mask_sem, far_sem, near_sem, power_sem, ref_sem,
):
    _, rows, cols = mask_ref.shape
    span, blocks, depth, _ = scene.shape
    half = depth // 2
    long_depth = refs.shape[3]
    long_dates = powers.shape[2]
    total_rows = rows * n
    stride = blocks * rows
    me = lax.axis_index("row")
    odd = lax.rem(me, 2)
    near = me + 1 - 2 * odd
    far = me - 1 + 2 * odd
    has_near = near < n
    has_far = (far >= 0) & (far < n)
    first_row = me * rows

    def peer(k):
        return lax.rem(me + k, n)

    def place(q):
        return q + odd * (rows - 1 - 2 * q)

    barrier = pltpu.get_barrier_semaphore()

    @pl.loop(1, n)
    def _(k):
        pl.semaphore_signal(barrier, inc=1, device_id={"row": peer(k)}, device_id_type=MESH)

    load = pltpu.make_async_copy(x_hbm, raw, load_sem)
    load.start()
    load_mask = pltpu.make_async_copy(mask_hbm, mask_ref, mask_sem)
    load_mask.start()
    column[...] = jnp.zeros_like(column)

    load.wait()
    wide[0:raw.shape[0], :] = raw[...].astype(jnp.float32)
    sums = jnp.zeros((half, LANE), jnp.float32)
    dates = lax.broadcasted_iota(jnp.int32, (half, LANE), 0)
    for q in range(rows):
        for part in range(2):
            for block in range(blocks):
                start = part * ndate * stride + block * rows + place(q)
                piece = wide[pl.ds(start, half, stride=stride), :]
                piece = jnp.where(dates < ndate, piece, 0.0)
                scene[HALF + q, block, part * half:(part + 1) * half, :] = piece.astype(jnp.bfloat16)
                sums = sums + piece * piece
    column[0:half, :] = sums
    powers[me] = jnp.sum(column[0:long_dates, :].T, axis=0, keepdims=True)

    pl.semaphore_wait(barrier, n - 1)

    def exchange(buffer, sems):
        def copy(k, slot):
            return pltpu.make_async_remote_copy(
                src_ref=buffer.at[slot], dst_ref=buffer.at[slot],
                send_sem=sems.at[0, k], recv_sem=sems.at[1, slot],
                device_id={"row": peer(k)}, device_id_type=MESH,
            )

        def start():
            @pl.loop(1, n)
            def _(k):
                copy(k, me).start()

        def finish():
            @pl.loop(1, n)
            def _(k):
                copy(k, peer(k)).wait_recv()

            @pl.loop(1, n)
            def _(k):
                copy(k, me).wait_send()

        return start, finish

    start_power, finish_power = exchange(powers, power_sem)
    start_power()

    far_id = jnp.clip(far, 0, n - 1)
    near_id = jnp.clip(near, 0, n - 1)

    def far_copy(t):
        return pltpu.make_async_remote_copy(
            src_ref=scene.at[HALF + t], dst_ref=scene.at[HALF - 1 - t],
            send_sem=far_sem.at[0, t], recv_sem=far_sem.at[1, t],
            device_id={"row": far_id}, device_id_type=MESH,
        )

    def near_copy(t):
        return pltpu.make_async_remote_copy(
            src_ref=scene.at[HALF + rows - 1 - t], dst_ref=scene.at[HALF + rows + t],
            send_sem=near_sem.at[0, t], recv_sem=near_sem.at[1, t],
            device_id={"row": near_id}, device_id_type=MESH,
        )

    for t in range(HALF):
        pl.when(has_far)(far_copy(t).start)
    for t in range(HALF):
        pl.when(has_near)(near_copy(t).start)

    @pl.when(jnp.logical_not(has_far))
    def _():
        scene[0:HALF] = jnp.zeros((HALF, blocks, depth, LANE), scene.dtype)

    @pl.when(jnp.logical_not(has_near))
    def _():
        scene[HALF + rows:span] = jnp.zeros((HALF, blocks, depth, LANE), scene.dtype)

    load_mask.wait()
    row_ids = first_row + lax.broadcasted_iota(jnp.int32, (rows, cols), 0)
    col_ids = lax.broadcasted_iota(jnp.int32, (rows, cols), 1)
    count = jnp.zeros((rows, cols), jnp.float32)
    ones = []
    for a in range(WIDTH):
        step = a + odd * (WIDTH - 1 - 2 * a)
        for b in range(WIDTH):
            there = row_ids + (step - HALF)
            inside = (there >= 0) & (there < total_rows)
            inside = inside & (col_ids + (b - HALF) >= 0) & (col_ids + (b - HALF) < cols)
            if (a, b) != (HALF, HALF):
                inside = inside & (mask_ref[step * WIDTH + b] == 1)
            one = inside.astype(jnp.float32)
            ones.append(one)
            count = count + one
    inverse = 1.0 / (count * ndate)
    for o in range(WIDTH * WIDTH):
        line = ones[o] * inverse
        for q in range(rows):
            chosen[q, o:o + 1, :] = jnp.where(odd == 1, line[rows - 1 - q:rows - q], line[q:q + 1])
    for q in range(rows):
        chosen[q, WIDTH * WIDTH:, :] = jnp.zeros((chosen.shape[1] - WIDTH * WIDTH, cols), jnp.float32)

    def window(block):
        return max(0, block * LANE - SUB), min(cols, (block + 1) * LANE + SUB)

    coef[...] = jnp.zeros_like(coef)
    for block in range(blocks):
        begin, end = window(block)
        shape = (end - begin, LANE)
        shift = begin - block * LANE
        shift = shift + lax.broadcasted_iota(jnp.int32, shape, 0) - lax.broadcasted_iota(jnp.int32, shape, 1)
        for q in range(rows):
            for a in range(WIDTH):
                band = jnp.zeros(shape, jnp.float32)
                for b in range(WIDTH):
                    line = chosen[q, a * WIDTH + b:a * WIDTH + b + 1, block * LANE:(block + 1) * LANE]
                    band = jnp.where(shift == b - HALF, line, band)
                weight[block, q, a, 0:end - begin, :] = band

    target = index_ref[0]
    target_row = lax.div(target, cols) - first_row
    target_col = lax.rem(target, cols)
    base = jnp.clip(lax.div(target_col + SUB - HALF, SUB) - 1, 0, cols // SUB - 2)
    home = lax.broadcasted_iota(jnp.int32, (1, long_depth), 1) * 0 + target_row

    def turn(slot):
        for block in range(blocks):
            tall = jnp.concatenate(
                [scene[slot, block], jnp.zeros((long_depth - depth, LANE), scene.dtype)], axis=0
            )
            turned[slot, block * LANE:(block + 1) * LANE, :] = tall.T
        first = jnp.zeros((SUB, long_depth), scene.dtype)
        second = first
        group = lax.broadcasted_iota(jnp.int32, (SUB, long_depth), 1) * 0 + base
        for k in range(cols // SUB):
            piece = turned[slot, k * SUB:(k + 1) * SUB, :]
            first = first + piece * (group == k).astype(jnp.float32).astype(scene.dtype)
            second = second + piece * (group == k - 1).astype(jnp.float32).astype(scene.dtype)
        picks[slot, 0:SUB, :] = first
        picks[slot, SUB:2 * SUB, :] = second

    for q in range(rows):
        turn(HALF + q)

    finish_power()
    power = jnp.sum(powers[...], axis=0)
    gain_row = lax.rsqrt(power * (1.0 / (total_rows * cols)) + 0.1)
    gains[...] = jnp.broadcast_to(gain_row, (LANE, long_dates)).T[0:half, :]
    tall = jnp.concatenate([gains[...], gains[...], jnp.zeros((long_depth - depth, LANE), jnp.float32)], axis=0)
    long_gain[...] = tall.T[0:8, :]

    def set_pair(q, block, real, imag):
        pairs[q, block, 0:half, 0:LANE] = real
        pairs[q, block, 0:half, LANE:2 * LANE] = imag
        pairs[q, block, half:depth, 0:LANE] = imag
        pairs[q, block, half:depth, LANE:2 * LANE] = -real

    for q in range(rows):
        for block in range(blocks):
            square = gains[...] * gains[...]
            tile = scene[HALF + q, block].astype(jnp.float32)
            set_pair(
                q, block, (tile[0:half] * square).astype(jnp.bfloat16), (tile[half:depth] * square).astype(jnp.bfloat16)
            )

    def project(q, block, slots):
        begin, end = window(block)
        size = end - begin
        left = jnp.concatenate([turned[slot, begin:end, 0:depth] for slot in slots], axis=0)
        proj = jnp.dot(left, pairs[q, block], preferred_element_type=jnp.float32)
        for i, slot in enumerate(slots):
            a = slot - q
            band = weight[block, q, a, 0:size, :]
            both = jnp.concatenate([band, band], axis=1)
            part = proj[i * size:(i + 1) * size] * both
            coef[q, block, a * cols + begin:a * cols + end, :] = part.astype(jnp.bfloat16)

    def update(q, block, slots):
        left = jnp.concatenate([scene[s, b] for s in slots for b in range(blocks)], axis=1)
        right = coef[q, block, (slots[0] - q) * cols:(slots[-1] + 1 - q) * cols, :]
        return jnp.dot(left, right, preferred_element_type=jnp.float32)

    def normalize(product):
        gain = gains[...]
        top, bottom = product[0:half], product[half:depth]
        real = (top[:, 0:LANE] - bottom[:, LANE:2 * LANE]) * gain
        imag = (top[:, LANE:2 * LANE] + bottom[:, 0:LANE]) * gain
        energy = jnp.sum(real * real + imag * imag, axis=0, keepdims=True)
        factor = lax.rsqrt(energy * (1.0 / ndate) + 0.001)
        return real * factor, imag * factor

    def rest(q, block, product):
        real, imag = normalize(product)
        for _ in range(1, ITERS):
            gain = gains[...]
            set_pair(q, block, (real * gain).astype(jnp.bfloat16), (imag * gain).astype(jnp.bfloat16))
            project(q, block, list(range(q, q + WIDTH)))
            real, imag = normalize(update(q, block, list(range(q, q + WIDTH))))
        vectors[q, block, 0:half, :] = real
        vectors[q, block, half:depth, :] = imag

    def seen(q, slots):
        return [s for s in slots if q <= s < q + WIDTH]

    for t in range(HALF):
        pl.when(has_near)(near_copy(t).wait_recv)
        turn(HALF + rows + t)
    for q in range(rows):
        for block in range(blocks):
            project(q, block, seen(q, range(HALF, span)))

    def whole(q, block):
        rest(q, block, update(q, block, list(range(q, q + WIDTH))))

    def swap(x):
        lanes = lax.broadcasted_iota(jnp.int32, x.shape, 1)
        ahead = pltpu.roll(x, long_depth - half, 1)
        behind = pltpu.roll(x, half, 1)
        return jnp.where(lanes < half, -ahead, jnp.where(lanes < depth, behind, 0.0))

    def reference_vector(q):
        shape = (2 * SUB, WIDTH * 2 * SUB)
        offset = lax.broadcasted_iota(jnp.int32, shape, 0)
        line = lax.broadcasted_iota(jnp.int32, shape, 1)
        hit = line - (offset // WIDTH) * (2 * SUB) == target_col - HALF - base * SUB + offset % WIDTH
        hit = hit & (line // (2 * SUB) == offset // WIDTH)
        left = hit.astype(jnp.float32).astype(jnp.bfloat16)
        right = jnp.concatenate([picks[q + a] for a in range(WIDTH)], axis=0)
        stack = jnp.dot(left, right, preferred_element_type=jnp.float32)
        lanes = lax.broadcasted_iota(jnp.int32, (2 * SUB, cols), 1)
        bands = jnp.sum(jnp.where(lanes == target_col, chosen[q], 0.0), axis=1, keepdims=True)
        middle = HALF * WIDTH + HALF
        center = stack[middle:middle + 1]
        gain = long_gain[0:1, :]
        vector = center * gain
        for _ in range(ITERS):
            vector = vector * gain
            proj_real = jnp.sum(stack * vector, axis=1, keepdims=True) * bands
            proj_imag = jnp.sum(stack * -swap(vector), axis=1, keepdims=True) * bands
            vector = jnp.sum(stack * proj_real, axis=0, keepdims=True)
            vector = vector + swap(jnp.sum(stack * proj_imag, axis=0, keepdims=True))
            vector = vector * gain
            energy = jnp.sum(vector * vector, axis=1, keepdims=True)
            vector = vector * lax.rsqrt(energy * (1.0 / ndate) + 0.001)
        return vector

    finish = []

    def send_reference(q):
        refs[q, me] = jnp.where(home == place(q), reference_vector(q), 0.0)
        start, end = exchange(refs.at[q], ref_sem.at[q])
        start()
        finish.append(end)

    for q in range(HALF, rows):
        send_reference(q)
        for block in range(blocks):
            whole(q, block)
    for t in range(HALF):
        slot = HALF - 1 - t
        pl.when(has_far)(far_copy(t).wait_recv)
        turn(slot)
        if slot < rows:
            send_reference(slot)
        for q in range(min(slot, rows - 1), -1, -1):
            for block in range(blocks):
                project(q, block, [slot])
        for block in range(blocks):
            if slot > 0:
                if slot < rows:
                    whole(slot, block)
                if slot == 1:
                    total[0, block] = update(0, block, list(range(1, WIDTH)))
            else:
                rest(0, block, total[0, block] + update(0, block, [0]))

    for end in finish:
        end()
    refvec = jnp.sum(jnp.sum(refs[...], axis=0), axis=0)
    refvec = jnp.broadcast_to(refvec, (LANE, long_depth)).T
    ref_real = refvec[0:half]
    ref_imag = refvec[half:depth]
    for q in range(rows):
        for block in range(blocks):
            real = vectors[q, block, 0:half, :]
            imag = vectors[q, block, half:depth, :]
            start = block * rows + place(q)
            out_ref[pl.ds(start, ndate, stride=stride), :] = (real * ref_real + imag * ref_imag)[0:ndate]
            start = start + ndate * stride
            out_ref[pl.ds(start, ndate, stride=stride), :] = (imag * ref_real - real * ref_imag)[0:ndate]

    for t in range(HALF):
        pl.when(has_far)(far_copy(t).wait_send)
        pl.when(has_near)(near_copy(t).wait_send)


def per_device(slc, mask, ref_index):
    parts, ndate, rows, cols = slc.shape
    n = lax.axis_size("row")
    half = round_up(ndate, SUB)
    depth = 2 * half
    long_dates = round_up(half, LANE)
    long_depth = round_up(depth, LANE)
    blocks = cols // LANE
    span = rows + 2 * HALF
    lines = parts * ndate * blocks * rows
    x = slc.reshape(parts, ndate, rows, blocks, LANE).transpose(0, 1, 3, 2, 4).reshape(lines, LANE)
    vmem = pl.BlockSpec(memory_space=pltpu.VMEM)
    anywhere = pl.BlockSpec(memory_space=pltpu.HBM)

    def body(*refs):
        kernel(n, ndate, *refs)

    out = pl.pallas_call(
        body,
        out_shape=jax.ShapeDtypeStruct((lines, LANE), jnp.float32),
        in_specs=[anywhere, anywhere, pl.BlockSpec(memory_space=pltpu.SMEM)],
        out_specs=vmem,
        scratch_shapes=[
            pltpu.VMEM((lines, LANE), jnp.bfloat16),
            pltpu.VMEM(mask.shape, jnp.int32),
            pltpu.VMEM((lines + (half - ndate) * blocks * rows, LANE), jnp.float32),
            pltpu.VMEM((span, blocks, depth, LANE), jnp.bfloat16),
            pltpu.VMEM((span, cols, long_depth), jnp.bfloat16),
            pltpu.VMEM((rows, 2 * SUB, cols), jnp.float32),
            pltpu.VMEM((span, 2 * SUB, long_depth), jnp.bfloat16),
            pltpu.VMEM((blocks, rows, WIDTH, LANE + 2 * SUB, LANE), jnp.float32),
            pltpu.VMEM((rows, blocks, depth, 2 * LANE), jnp.bfloat16),
            pltpu.VMEM((rows, blocks, WIDTH * cols, 2 * LANE), jnp.bfloat16),
            pltpu.VMEM((rows, blocks, depth, 2 * LANE), jnp.float32),
            pltpu.VMEM((rows, blocks, depth, LANE), jnp.float32),
            pltpu.VMEM((half, LANE), jnp.float32),
            pltpu.VMEM((8, long_depth), jnp.float32),
            pltpu.VMEM((long_depth, LANE), jnp.float32),
            pltpu.VMEM((n, 1, long_dates), jnp.float32),
            pltpu.VMEM((rows, n, 1, long_depth), jnp.float32),
            pltpu.SemaphoreType.DMA,
            pltpu.SemaphoreType.DMA,
            pltpu.SemaphoreType.DMA((2, HALF)),
            pltpu.SemaphoreType.DMA((2, HALF)),
            pltpu.SemaphoreType.DMA((2, n)),
            pltpu.SemaphoreType.DMA((rows, 2, n)),
        ],
        compiler_params=pltpu.CompilerParams(collective_id=0, has_side_effects=True, vmem_limit_bytes=VMEM_LIMIT),
        name="link",
    )(pltpu.with_memory_space_constraint(x, pltpu.HBM), pltpu.with_memory_space_constraint(mask, pltpu.HBM), ref_index)

    def put(in_ref, out_ref, sem):
        copy = pltpu.make_async_copy(in_ref, out_ref, sem)
        copy.start()
        copy.wait()

    out = pl.pallas_call(
        put,
        out_shape=jax.ShapeDtypeStruct((lines, LANE), jnp.float32),
        in_specs=[vmem],
        out_specs=anywhere,
        scratch_shapes=[pltpu.SemaphoreType.DMA],
        compiler_params=pltpu.CompilerParams(vmem_limit_bytes=16 * 1024 * 1024),
        name="put",
    )(out)
    out = out.reshape(parts, ndate, blocks, rows, LANE).transpose(0, 1, 3, 2, 4)
    return out.reshape(parts, ndate, rows, cols)


def solution(mesh):
    placed = (P(None, None, ("grp", "row"), None), P(None, ("grp", "row"), None), P("grp"))
    return jax.shard_map(
        per_device,
        mesh=mesh,
        in_specs=placed,
        out_specs=P(None, None, ("grp", "row"), None),
        check_vma=False,
    )
```

```python
import jax
import jax.numpy as jnp
from jax import lax
from jax.experimental import pallas as pl
from jax.experimental.pallas import tpu as pltpu
from jax.sharding import PartitionSpec as P

HALF = 2
ITERS = 2
WIDTH = 2 * HALF + 1
LANE = 128
SUB = 16
VMEM_LIMIT = 32000000
MESH = pl.DeviceIdType.MESH


def round_up(value, unit):
    return (value + unit - 1) // unit * unit


def kernel(
    n, ndate, x_hbm, mask_hbm, index_ref, out_ref,
    raw, mask_ref, wide, scene, turned, chosen, picks, weight, pairs, coef, late, edges, total, vectors, gains, long_gain, column, powers, refs,
    load_sem, mask_sem, far_sem, near_sem, power_sem, ref_sem,
):
    _, rows, cols = mask_ref.shape
    span, blocks, depth, _ = scene.shape
    half = depth // 2
    tiles = turned.shape[1]
    long_depth = refs.shape[3]
    long_dates = powers.shape[2]
    total_rows = rows * n
    stride = blocks * rows
    me = lax.axis_index("row")
    odd = lax.rem(me, 2)
    near = me + 1 - 2 * odd
    far = me - 1 + 2 * odd
    has_near = near < n
    has_far = (far >= 0) & (far < n)
    first_row = me * rows

    def peer(k):
        return lax.rem(me + k, n)

    def place(q):
        return q + odd * (rows - 1 - 2 * q)

    barrier = pltpu.get_barrier_semaphore()

    @pl.loop(1, n)
    def _(k):
        pl.semaphore_signal(barrier, inc=1, device_id={"row": peer(k)}, device_id_type=MESH)

    load = pltpu.make_async_copy(x_hbm, raw, load_sem)
    load.start()
    load_mask = pltpu.make_async_copy(mask_hbm, mask_ref, mask_sem)
    load_mask.start()
    column[...] = jnp.zeros_like(column)

    load.wait()
    wide[0:raw.shape[0], :] = raw[...].astype(jnp.float32)
    sums = jnp.zeros((half, LANE), jnp.float32)
    dates = lax.broadcasted_iota(jnp.int32, (half, LANE), 0)
    for q in range(rows):
        for part in range(2):
            for block in range(blocks):
                start = part * ndate * stride + block * rows + place(q)
                piece = wide[pl.ds(start, half, stride=stride), :]
                piece = jnp.where(dates < ndate, piece, 0.0)
                scene[HALF + q, block, part * half:(part + 1) * half, :] = piece.astype(jnp.bfloat16)
                sums = sums + piece * piece
    column[0:half, :] = sums
    powers[me] = jnp.sum(column[0:long_dates, :].T, axis=0, keepdims=True)

    pl.semaphore_wait(barrier, n - 1)

    def exchange(buffer, sems):
        def copy(k, slot):
            return pltpu.make_async_remote_copy(
                src_ref=buffer.at[slot], dst_ref=buffer.at[slot],
                send_sem=sems.at[0, k], recv_sem=sems.at[1, slot],
                device_id={"row": peer(k)}, device_id_type=MESH,
            )

        def start():
            for k in range(1, n):
                copy(k, me).start()

        def finish():
            @pl.loop(1, n)
            def _(k):
                copy(k, peer(k)).wait_recv()

            @pl.loop(1, n)
            def _(k):
                copy(k, me).wait_send()

        return start, finish

    start_power, finish_power = exchange(powers, power_sem)
    start_power()

    far_id = jnp.clip(far, 0, n - 1)
    near_id = jnp.clip(near, 0, n - 1)

    def far_copy(t):
        return pltpu.make_async_remote_copy(
            src_ref=scene.at[HALF + t], dst_ref=scene.at[HALF - 1 - t],
            send_sem=far_sem.at[0, t], recv_sem=far_sem.at[1, t],
            device_id={"row": far_id}, device_id_type=MESH,
        )

    def near_copy(t):
        return pltpu.make_async_remote_copy(
            src_ref=scene.at[HALF + rows - 1 - t], dst_ref=scene.at[HALF + rows + t],
            send_sem=near_sem.at[0, t], recv_sem=near_sem.at[1, t],
            device_id={"row": near_id}, device_id_type=MESH,
        )

    for t in range(HALF):
        pl.when(has_far)(far_copy(t).start)
    for t in range(HALF):
        pl.when(has_near)(near_copy(t).start)

    @pl.when(jnp.logical_not(has_far))
    def _():
        scene[0:HALF] = jnp.zeros((HALF, blocks, depth, LANE), scene.dtype)

    @pl.when(jnp.logical_not(has_near))
    def _():
        scene[HALF + rows:span] = jnp.zeros((HALF, blocks, depth, LANE), scene.dtype)

    load_mask.wait()
    row_ids = first_row + lax.broadcasted_iota(jnp.int32, (rows, cols), 0)
    col_ids = lax.broadcasted_iota(jnp.int32, (rows, cols), 1)
    count = jnp.zeros((rows, cols), jnp.float32)
    ones = []
    for a in range(WIDTH):
        step = a + odd * (WIDTH - 1 - 2 * a)
        for b in range(WIDTH):
            there = row_ids + (step - HALF)
            inside = (there >= 0) & (there < total_rows)
            inside = inside & (col_ids + (b - HALF) >= 0) & (col_ids + (b - HALF) < cols)
            if (a, b) != (HALF, HALF):
                inside = inside & (mask_ref[step * WIDTH + b] == 1)
            one = inside.astype(jnp.float32)
            ones.append(one)
            count = count + one
    inverse = 1.0 / (count * ndate)
    for o in range(WIDTH * WIDTH):
        line = ones[o] * inverse
        for q in range(rows):
            chosen[q, o:o + 1, :] = jnp.where(odd == 1, line[rows - 1 - q:rows - q], line[q:q + 1])
    for q in range(rows):
        chosen[q, WIDTH * WIDTH:, :] = jnp.zeros((chosen.shape[1] - WIDTH * WIDTH, cols), jnp.float32)

    def window(block):
        return max(0, block * LANE - SUB), min(cols, (block + 1) * LANE + SUB)

    coef[...] = jnp.zeros_like(coef)
    late[...] = jnp.zeros_like(late)
    for block in range(blocks):
        begin, end = window(block)
        shape = (end - begin, LANE)
        shift = begin - block * LANE
        shift = shift + lax.broadcasted_iota(jnp.int32, shape, 0) - lax.broadcasted_iota(jnp.int32, shape, 1)
        for q in range(rows):
            for a in range(WIDTH):
                band = jnp.zeros(shape, jnp.float32)
                for b in range(WIDTH):
                    line = chosen[q, a * WIDTH + b:a * WIDTH + b + 1, block * LANE:(block + 1) * LANE]
                    band = jnp.where(shift == b - HALF, line, band)
                weight[block, q, a, 0:end - begin, :] = band

    target = index_ref[0]
    target_row = lax.div(target, cols) - first_row
    target_col = lax.rem(target, cols)
    base = jnp.clip(lax.div(target_col + SUB - HALF, SUB) - 1, 0, cols // SUB - 2)
    home = lax.broadcasted_iota(jnp.int32, (1, long_depth), 1) * 0 + target_row

    def turn(slot):
        for block in range(blocks):
            lines = slice(block * LANE, (block + 1) * LANE)
            for i in range(tiles):
                deep = slice(i * LANE, min((i + 1) * LANE, depth))
                tile = scene[slot, block, deep, :]
                if tile.shape[0] < LANE:
                    tile = jnp.concatenate([tile, jnp.zeros((LANE - tile.shape[0], LANE), tile.dtype)], axis=0)
                turned[slot, i, lines, :] = tile.T
        group = lax.broadcasted_iota(jnp.int32, (SUB, LANE), 1) * 0 + base
        hits = [(group == k).astype(jnp.float32).astype(scene.dtype) for k in range(-1, cols // SUB)]
        for i in range(tiles):
            first = jnp.zeros((SUB, LANE), scene.dtype)
            second = first
            for k in range(cols // SUB):
                piece = turned[slot, i, k * SUB:(k + 1) * SUB, :]
                first = first + piece * hits[k + 1]
                second = second + piece * hits[k]
            picks[slot, i, 0:SUB, :] = first
            picks[slot, i, SUB:2 * SUB, :] = second

    def sides(block):
        ends = []
        if block > 0:
            ends.append(block * LANE - SUB)
        if block < blocks - 1:
            ends.append((block + 1) * LANE)
        return ends

    def set_edges(low):
        for block in range(blocks):
            for i in range(tiles):
                parts = []
                for end in sides(block):
                    if low > 0:
                        parts.append(jnp.zeros((low * SUB, LANE), edges.dtype))
                    for slot in range(low, span):
                        parts.append(turned[slot, i, end:end + SUB, :])
                used = len(sides(block)) * span * SUB
                if used < edges.shape[2]:
                    parts.append(jnp.zeros((edges.shape[2] - used, LANE), edges.dtype))
                edges[block, i * LANE:(i + 1) * LANE, :] = jnp.concatenate(parts, axis=0).T

    for q in range(rows):
        turn(HALF + q)

    finish_power()
    power = jnp.sum(powers[...], axis=0)
    gain_row = lax.rsqrt(power * (1.0 / (total_rows * cols)) + 0.1)
    gains[...] = jnp.broadcast_to(gain_row, (LANE, long_dates)).T[0:half, :]
    tall = jnp.concatenate([gains[...], gains[...], jnp.zeros((long_depth - depth, LANE), jnp.float32)], axis=0)
    long_gain[...] = tall.T[0:8, :]

    def set_pair(q, block, real, imag):
        pairs[q, block, 0, 0:half, :] = real
        pairs[q, block, 1, 0:half, :] = imag
        pairs[q, block, 0, half:depth, :] = imag
        pairs[q, block, 1, half:depth, :] = -real

    for q in range(rows):
        for block in range(blocks):
            square = gains[...] * gains[...]
            tile = scene[HALF + q, block].astype(jnp.float32)
            set_pair(
                q, block, (tile[0:half] * square).astype(jnp.bfloat16), (tile[half:depth] * square).astype(jnp.bfloat16)
            )

    def project(q, block, slots, into_late=False):
        begin, end = window(block)
        size = end - begin
        main = block * LANE - begin
        left = jnp.concatenate(
            [jnp.concatenate([turned[slot, i, begin:end, :] for i in range(tiles)], axis=1) for slot in slots], axis=0
        )
        right = jnp.concatenate([pairs[q, block, 0], pairs[q, block, 1]], axis=1)
        proj = jnp.dot(left[:, 0:depth], right, preferred_element_type=jnp.float32)
        for i, slot in enumerate(slots):
            a = slot - q
            band = weight[block, q, a, 0:size, :]
            for c in range(2):
                part = (proj[i * size:(i + 1) * size, c * LANE:(c + 1) * LANE] * band).astype(jnp.bfloat16)
                if into_late:
                    late[q, block, c, begin:end, :] = part
                    continue
                coef[q, block, c, a * LANE:(a + 1) * LANE, :] = part[main:main + LANE]
                for k, side in enumerate(sides(block)):
                    spot = WIDTH * LANE + (k * span + slot) * SUB
                    coef[q, block, c, spot:spot + SUB, :] = part[side - begin:side - begin + SUB]

    def update(q, block, slots):
        left = jnp.concatenate([scene[s, block] for s in slots] + [edges[block, 0:depth, :]], axis=1)
        first = (slots[0] - q) * LANE
        right = jnp.concatenate([coef[q, block, 0, first:, :], coef[q, block, 1, first:, :]], axis=1)
        return jnp.dot(left, right, preferred_element_type=jnp.float32)

    def late_update(q, block, slot):
        left = jnp.concatenate([scene[slot, b] for b in range(blocks)], axis=1)
        right = jnp.concatenate([late[q, block, 0], late[q, block, 1]], axis=1)
        return jnp.dot(left, right, preferred_element_type=jnp.float32)

    def normalize(product):
        gain = gains[...]
        top, bottom = product[0:half], product[half:depth]
        real = (top[:, 0:LANE] - bottom[:, LANE:2 * LANE]) * gain
        imag = (top[:, LANE:2 * LANE] + bottom[:, 0:LANE]) * gain
        energy = jnp.sum(real * real + imag * imag, axis=0, keepdims=True)
        factor = lax.rsqrt(energy * (1.0 / ndate) + 0.001)
        return real * factor, imag * factor

    def first_step(q, block, product):
        real, imag = normalize(product)
        gain = gains[...]
        set_pair(q, block, (real * gain).astype(jnp.bfloat16), (imag * gain).astype(jnp.bfloat16))

    def last_steps(q):
        window_slots = list(range(q, q + WIDTH))
        for i in range(1, ITERS):
            for block in range(blocks):
                project(q, block, window_slots)
            products = [update(q, block, window_slots) for block in range(blocks)]
            for block in range(blocks):
                real, imag = normalize(products[block])
                if i < ITERS - 1:
                    gain = gains[...]
                    set_pair(q, block, (real * gain).astype(jnp.bfloat16), (imag * gain).astype(jnp.bfloat16))
                else:
                    vectors[q, block, 0:half, :] = real
                    vectors[q, block, half:depth, :] = imag

    def seen(q, slots):
        return [s for s in slots if q <= s < q + WIDTH]

    for t in range(HALF):
        pl.when(has_near)(near_copy(t).wait_recv)
        turn(HALF + rows + t)
    set_edges(HALF)
    for q in range(rows):
        slots = seen(q, range(HALF, span))
        for block in range(blocks):
            project(q, block, slots)
        for block in range(blocks):
            total[q, block] = update(q, block, slots)

    def swap(x):
        lanes = lax.broadcasted_iota(jnp.int32, x.shape, 1)
        ahead = pltpu.roll(x, long_depth - half, 1)
        behind = pltpu.roll(x, half, 1)
        return jnp.where(lanes < half, -ahead, jnp.where(lanes < depth, behind, 0.0))

    def reference_vector(q):
        shape = (2 * SUB, WIDTH * 2 * SUB)
        offset = lax.broadcasted_iota(jnp.int32, shape, 0)
        line = lax.broadcasted_iota(jnp.int32, shape, 1)
        hit = line - (offset // WIDTH) * (2 * SUB) == target_col - HALF - base * SUB + offset % WIDTH
        hit = hit & (line // (2 * SUB) == offset // WIDTH)
        left = hit.astype(jnp.float32).astype(jnp.bfloat16)
        right = jnp.concatenate(
            [jnp.concatenate([picks[q + a, i] for i in range(tiles)], axis=1) for a in range(WIDTH)], axis=0
        )
        stack = jnp.dot(left, right, preferred_element_type=jnp.float32)
        lanes = lax.broadcasted_iota(jnp.int32, (2 * SUB, cols), 1)
        bands = jnp.sum(jnp.where(lanes == target_col, chosen[q], 0.0), axis=1, keepdims=True)
        middle = HALF * WIDTH + HALF
        center = stack[middle:middle + 1]
        gain = long_gain[0:1, :]
        vector = center * gain
        for _ in range(ITERS):
            vector = vector * gain
            proj_real = jnp.sum(stack * vector, axis=1, keepdims=True) * bands
            proj_imag = jnp.sum(stack * -swap(vector), axis=1, keepdims=True) * bands
            vector = jnp.sum(stack * proj_real, axis=0, keepdims=True)
            vector = vector + swap(jnp.sum(stack * proj_imag, axis=0, keepdims=True))
            vector = vector * gain
            energy = jnp.sum(vector * vector, axis=1, keepdims=True)
            vector = vector * lax.rsqrt(energy * (1.0 / ndate) + 0.001)
        return vector

    finish = []

    def set_reference(q):
        refs[q, me] = jnp.where(home == place(q), reference_vector(q), 0.0)

    def send_reference(q):
        start, end = exchange(refs.at[q], ref_sem.at[q])
        start()
        finish.append(end)

    for q in range(HALF, rows):
        set_reference(q)
        send_reference(q)
        for block in range(blocks):
            first_step(q, block, total[q, block])
        last_steps(q)
    for t in range(HALF):
        slot = HALF - 1 - t
        pl.when(has_far)(far_copy(t).wait_recv)
        turn(slot)
        set_edges(slot)
        if slot < rows:
            set_reference(slot)
        for q in range(min(slot, rows - 1), -1, -1):
            for block in range(blocks):
                project(q, block, [slot], into_late=True)
        if slot < rows:
            products = [late_update(slot, block, slot) for block in range(blocks)]
            for block in range(blocks):
                first_step(slot, block, total[slot, block] + products[block])
            send_reference(slot)
            last_steps(slot)
        for q in range(min(slot, rows) - 1, -1, -1):
            for block in range(blocks):
                total[q, block] += late_update(q, block, slot)

    for end in finish:
        end()
    refvec = jnp.sum(jnp.sum(refs[...], axis=0), axis=0)
    refvec = jnp.broadcast_to(refvec, (LANE, long_depth)).T
    ref_real = refvec[0:half]
    ref_imag = refvec[half:depth]
    for q in range(rows):
        for block in range(blocks):
            real = vectors[q, block, 0:half, :]
            imag = vectors[q, block, half:depth, :]
            start = block * rows + place(q)
            out_ref[pl.ds(start, ndate, stride=stride), :] = (real * ref_real + imag * ref_imag)[0:ndate]
            start = start + ndate * stride
            out_ref[pl.ds(start, ndate, stride=stride), :] = (imag * ref_real - real * ref_imag)[0:ndate]

    for t in range(HALF):
        pl.when(has_far)(far_copy(t).wait_send)
        pl.when(has_near)(near_copy(t).wait_send)


def per_device(slc, mask, ref_index):
    parts, ndate, rows, cols = slc.shape
    n = lax.axis_size("row")
    half = round_up(ndate, SUB)
    depth = 2 * half
    long_dates = round_up(half, LANE)
    long_depth = round_up(depth, LANE)
    blocks = cols // LANE
    span = rows + 2 * HALF
    lines = parts * ndate * blocks * rows
    margin = round_up(min(2, blocks - 1) * span * SUB, LANE)
    x = slc.reshape(parts, ndate, rows, blocks, LANE).transpose(0, 1, 3, 2, 4).reshape(lines, LANE)
    vmem = pl.BlockSpec(memory_space=pltpu.VMEM)
    anywhere = pl.BlockSpec(memory_space=pltpu.HBM)

    def body(*refs):
        kernel(n, ndate, *refs)

    out = pl.pallas_call(
        body,
        out_shape=jax.ShapeDtypeStruct((lines, LANE), jnp.float32),
        in_specs=[anywhere, anywhere, pl.BlockSpec(memory_space=pltpu.SMEM)],
        out_specs=vmem,
        scratch_shapes=[
            pltpu.VMEM((lines, LANE), jnp.bfloat16),
            pltpu.VMEM(mask.shape, jnp.int32),
            pltpu.VMEM((lines + (half - ndate) * blocks * rows, LANE), jnp.float32),
            pltpu.VMEM((span, blocks, depth, LANE), jnp.bfloat16),
            pltpu.VMEM((span, long_depth // LANE, cols, LANE), jnp.bfloat16),
            pltpu.VMEM((rows, 2 * SUB, cols), jnp.float32),
            pltpu.VMEM((span, long_depth // LANE, 2 * SUB, LANE), jnp.bfloat16),
            pltpu.VMEM((blocks, rows, WIDTH, LANE + 2 * SUB, LANE), jnp.float32),
            pltpu.VMEM((rows, blocks, 2, depth, LANE), jnp.bfloat16),
            pltpu.VMEM((rows, blocks, 2, WIDTH * LANE + margin, LANE), jnp.bfloat16),
            pltpu.VMEM((rows, blocks, 2, cols, LANE), jnp.bfloat16),
            pltpu.VMEM((blocks, long_depth, margin), jnp.bfloat16),
            pltpu.VMEM((rows, blocks, depth, 2 * LANE), jnp.float32),
            pltpu.VMEM((rows, blocks, depth, LANE), jnp.float32),
            pltpu.VMEM((half, LANE), jnp.float32),
            pltpu.VMEM((8, long_depth), jnp.float32),
            pltpu.VMEM((long_depth, LANE), jnp.float32),
            pltpu.VMEM((n, 1, long_dates), jnp.float32),
            pltpu.VMEM((rows, n, 1, long_depth), jnp.float32),
            pltpu.SemaphoreType.DMA,
            pltpu.SemaphoreType.DMA,
            pltpu.SemaphoreType.DMA((2, HALF)),
            pltpu.SemaphoreType.DMA((2, HALF)),
            pltpu.SemaphoreType.DMA((2, n)),
            pltpu.SemaphoreType.DMA((rows, 2, n)),
        ],
        compiler_params=pltpu.CompilerParams(collective_id=0, has_side_effects=True, vmem_limit_bytes=VMEM_LIMIT),
        name="link",
    )(pltpu.with_memory_space_constraint(x, pltpu.HBM), pltpu.with_memory_space_constraint(mask, pltpu.HBM), ref_index)

    def put(in_ref, out_ref, sem):
        copy = pltpu.make_async_copy(in_ref, out_ref, sem)
        copy.start()
        copy.wait()

    out = pl.pallas_call(
        put,
        out_shape=jax.ShapeDtypeStruct((lines, LANE), jnp.float32),
        in_specs=[vmem],
        out_specs=anywhere,
        scratch_shapes=[pltpu.SemaphoreType.DMA],
        compiler_params=pltpu.CompilerParams(vmem_limit_bytes=16 * 1024 * 1024),
        name="put",
    )(out)
    out = out.reshape(parts, ndate, blocks, rows, LANE).transpose(0, 1, 3, 2, 4)
    return out.reshape(parts, ndate, rows, cols)


def solution(mesh):
    placed = (P(None, None, ("grp", "row"), None), P(None, ("grp", "row"), None), P("grp"))
    return jax.shard_map(
        per_device,
        mesh=mesh,
        in_specs=placed,
        out_specs=P(None, None, ("grp", "row"), None),
        check_vma=False,
    )
```

```python
import jax
import jax.numpy as jnp
from jax import lax
from jax.experimental import pallas as pl
from jax.experimental.pallas import tpu as pltpu
from jax.sharding import PartitionSpec as P

HALF = 2
ITERS = 2
WIDTH = 2 * HALF + 1
LANE = 128
SUB = 16
EIGHT = 8
GROUP = 4
VMEM_LIMIT = 32000000
MESH = pl.DeviceIdType.MESH


def round_up(value, unit):
    return (value + unit - 1) // unit * unit


def kernel(
    n, ndate, x_hbm, mask_hbm, index_ref, out_ref,
    raw, mask_ref, wide, scene, turned, chosen, picks, pieces, weight, pairs, coef, late, edges, total, vectors, gains, long_gain, column, powers, plane_rows, whole_row, refs,
    load_sem, mask_sem, lane_sem, far_sem, near_sem, piece_sem, power_sem, plane_sem, whole_sem, ref_sem,
):
    _, rows, cols = mask_ref.shape
    span, blocks, depth, _ = scene.shape
    half = depth // 2
    tiles = turned.shape[1]
    long_depth = refs.shape[2]
    long_dates = powers.shape[2]
    total_rows = rows * n
    stride = blocks * rows
    me = lax.axis_index("row")
    odd = lax.rem(me, 2)
    near = me + 1 - 2 * odd
    far = me - 1 + 2 * odd
    has_near = near < n
    has_far = (far >= 0) & (far < n)
    first_row = me * rows

    def peer(k):
        return lax.rem(me + k, n)

    def place(q):
        return q + odd * (rows - 1 - 2 * q)

    group = GROUP if n % GROUP == 0 else n
    planes = n // group
    plane = me // group
    lane = lax.rem(me, group)
    has_up = plane < planes - 1
    has_down = plane > 0
    crosses = has_far & ((lane + 1 - 2 * (1 - odd) < 0) | (lane + 1 - 2 * (1 - odd) > group - 1))

    def signal(sem, target):
        pl.semaphore_signal(sem, inc=1, device_id={"row": target}, device_id_type=MESH)

    def signal_mates(sem):
        for k in range(1, group):
            signal(sem, plane * group + lax.rem(lane + k, group))

    barrier = pltpu.get_barrier_semaphore()
    pl.when(crosses)(lambda: signal(barrier, jnp.clip(far, 0, n - 1)))
    pl.when(has_up)(lambda: signal(barrier, jnp.minimum(me + group, n - 1)))
    pl.when(has_down)(lambda: signal(barrier, jnp.maximum(me - group, 0)))
    signal_mates(barrier)
    expected = group - 1 + has_up.astype(jnp.int32) + has_down.astype(jnp.int32) + crosses.astype(jnp.int32)

    def meet_lane(d):
        pl.when(has_up)(lambda: signal(lane_sem.at[0, d], jnp.minimum(me + group, n - 1)))
        pl.when(has_down)(lambda: signal(lane_sem.at[1, d], jnp.maximum(me - group, 0)))

        @pl.when(has_down)
        def _():
            pl.semaphore_wait(lane_sem.at[0, d], 1)

        @pl.when(has_up)
        def _():
            pl.semaphore_wait(lane_sem.at[1, d], 1)

    load = pltpu.make_async_copy(x_hbm, raw, load_sem)
    load.start()
    load_mask = pltpu.make_async_copy(mask_hbm, mask_ref, mask_sem)
    load_mask.start()
    column[...] = jnp.zeros_like(column)

    load.wait()
    wide[0:raw.shape[0], :] = raw[...].astype(jnp.float32)
    sums = jnp.zeros((half, LANE), jnp.float32)
    dates = lax.broadcasted_iota(jnp.int32, (half, LANE), 0)
    for q in range(rows):
        for part in range(2):
            for block in range(blocks):
                start = part * ndate * stride + block * rows + place(q)
                piece = wide[pl.ds(start, half, stride=stride), :]
                piece = jnp.where(dates < ndate, piece, 0.0)
                scene[HALF + q, block, part * half:(part + 1) * half, :] = piece.astype(jnp.bfloat16)
                sums = sums + piece * piece
    column[0:half, :] = sums
    powers[lane] = jnp.sum(column[0:long_dates, :].T, axis=0, keepdims=True)

    target = index_ref[0]
    target_row = lax.div(target, cols) - first_row
    target_col = lax.rem(target, cols)
    base = jnp.clip(lax.div(target_col + SUB - HALF, SUB) - 1, 0, cols // SUB - 2)
    home = lax.broadcasted_iota(jnp.int32, (1, long_depth), 1) * 0 + target_row

    def turn(slot):
        for block in range(blocks):
            lines = slice(block * LANE, (block + 1) * LANE)
            for i in range(tiles):
                deep = slice(i * LANE, min((i + 1) * LANE, depth))
                tile = scene[slot, block, deep, :]
                if tile.shape[0] < LANE:
                    tile = jnp.concatenate([tile, jnp.zeros((LANE - tile.shape[0], LANE), tile.dtype)], axis=0)
                turned[slot, i, lines, :] = tile.T

    def pick(slot):
        group_of = lax.broadcasted_iota(jnp.int32, (SUB, LANE), 1) * 0 + base
        hits = [(group_of == k).astype(jnp.float32).astype(scene.dtype) for k in range(-1, cols // SUB)]
        strips = []
        for i in range(tiles):
            first = jnp.zeros((SUB, LANE), scene.dtype)
            second = first
            for k in range(cols // SUB):
                piece = turned[slot, i, k * SUB:(k + 1) * SUB, :]
                first = first + piece * hits[k + 1]
                second = second + piece * hits[k]
            strips.append(jnp.concatenate([first, second], axis=0))
        shape = (SUB, 2 * SUB)
        offset = lax.broadcasted_iota(jnp.int32, shape, 0)
        line = lax.broadcasted_iota(jnp.int32, shape, 1)
        hit = (line == target_col - HALF - base * SUB + offset) & (offset < WIDTH)
        left = hit.astype(jnp.float32).astype(scene.dtype)
        found = jnp.dot(left, jnp.concatenate(strips, axis=1), preferred_element_type=jnp.float32)
        picks[slot] = found[0:EIGHT].astype(scene.dtype)

    pl.semaphore_wait(barrier, expected)

    def mate_copy(k, rows_sent):
        return pltpu.make_async_remote_copy(
            src_ref=powers.at[rows_sent], dst_ref=powers.at[rows_sent],
            send_sem=power_sem.at[0], recv_sem=power_sem.at[1],
            device_id={"row": plane * group + lax.rem(lane + k, group)}, device_id_type=MESH,
        )

    def plane_copy(k, rows_sent):
        return pltpu.make_async_remote_copy(
            src_ref=plane_rows.at[rows_sent], dst_ref=plane_rows.at[rows_sent],
            send_sem=plane_sem.at[0], recv_sem=plane_sem.at[1],
            device_id={"row": lax.rem(plane + k, planes) * group + lane}, device_id_type=MESH,
        )

    def ref_copy(k, rows_sent):
        return pltpu.make_async_remote_copy(
            src_ref=refs.at[rows_sent], dst_ref=refs.at[rows_sent],
            send_sem=ref_sem.at[0], recv_sem=ref_sem.at[1],
            device_id={"row": peer(k)}, device_id_type=MESH,
        )

    mate_all = mate_copy(1, pl.ds(0, group - 1))
    ref_all = ref_copy(1, pl.ds(0, n - 1))
    if planes > 1:
        plane_all = plane_copy(1, pl.ds(0, planes - 1))

    inner = (lane > 0) & (lane < group - 1) if planes > 1 else lane >= 0
    outer = jnp.logical_not(inner)

    far_id = jnp.clip(far, 0, n - 1)
    near_id = jnp.clip(near, 0, n - 1)

    def far_copy(t, first, last):
        chunk = pl.ds(first, last - first)
        return pltpu.make_async_remote_copy(
            src_ref=scene.at[HALF + t, chunk], dst_ref=scene.at[HALF - 1 - t, chunk],
            send_sem=far_sem.at[HALF], recv_sem=far_sem.at[t],
            device_id={"row": far_id}, device_id_type=MESH,
        )

    def near_copy(t):
        return pltpu.make_async_remote_copy(
            src_ref=scene.at[HALF + rows - 1 - t], dst_ref=scene.at[HALF + rows + t],
            send_sem=near_sem.at[0], recv_sem=near_sem.at[1],
            device_id={"row": near_id}, device_id_type=MESH,
        )

    near_all = pltpu.make_async_remote_copy(
        src_ref=scene.at[pl.ds(HALF + rows - HALF, HALF)], dst_ref=scene.at[pl.ds(HALF + rows, HALF)],
        send_sem=near_sem.at[0], recv_sem=near_sem.at[1],
        device_id={"row": near_id}, device_id_type=MESH,
    )
    far_all = pltpu.make_async_remote_copy(
        src_ref=scene.at[pl.ds(HALF, HALF)], dst_ref=scene.at[pl.ds(0, HALF)],
        send_sem=far_sem.at[HALF], recv_sem=far_sem.at[0],
        device_id={"row": far_id}, device_id_type=MESH,
    )
    piece_copy = pltpu.make_async_remote_copy(
        src_ref=pieces, dst_ref=picks.at[pl.ds(0, HALF)],
        send_sem=piece_sem.at[0], recv_sem=piece_sem.at[1],
        device_id={"row": far_id}, device_id_type=MESH,
    )

    def send_rest():
        piece_copy.start()
        far_copy(0, 1, blocks).start()
        for t in range(1, HALF):
            far_copy(t, 0, blocks).start()

    whole_copy = pltpu.make_async_remote_copy(
        src_ref=whole_row, dst_ref=whole_row, send_sem=whole_sem.at[0], recv_sem=whole_sem.at[1],
        device_id={"row": near_id}, device_id_type=MESH,
    )
    for k in range(1, group):
        mate_copy(k, lane).start()
    pl.when(inner & has_far)(far_copy(0, 0, 1).start)
    for t in range(HALF):
        pl.when(has_near)(near_copy(t).start)
    for q in range(rows):
        turn(HALF + q)
        pick(HALF + q)
    for t in range(HALF):
        pieces[HALF - 1 - t] = picks[HALF + t]
    pl.when(inner & has_far)(send_rest)

    @pl.when(jnp.logical_not(has_far))
    def _():
        scene[0:HALF] = jnp.zeros((HALF, blocks, depth, LANE), scene.dtype)
        picks[0:HALF] = jnp.zeros((HALF, EIGHT, long_depth), scene.dtype)

    @pl.when(jnp.logical_not(has_near))
    def _():
        scene[HALF + rows:span] = jnp.zeros((HALF, blocks, depth, LANE), scene.dtype)

    load_mask.wait()
    row_ids = first_row + lax.broadcasted_iota(jnp.int32, (rows, cols), 0)
    col_ids = lax.broadcasted_iota(jnp.int32, (rows, cols), 1)
    count = jnp.zeros((rows, cols), jnp.float32)
    ones = []
    for a in range(WIDTH):
        step = a + odd * (WIDTH - 1 - 2 * a)
        for b in range(WIDTH):
            there = row_ids + (step - HALF)
            inside = (there >= 0) & (there < total_rows)
            inside = inside & (col_ids + (b - HALF) >= 0) & (col_ids + (b - HALF) < cols)
            if (a, b) != (HALF, HALF):
                inside = inside & (mask_ref[step * WIDTH + b] == 1)
            one = inside.astype(jnp.float32)
            ones.append(one)
            count = count + one
    inverse = 1.0 / (count * ndate)
    chosen[...] = jnp.zeros_like(chosen)
    for o in range(WIDTH * WIDTH):
        line = ones[o] * inverse
        for q in range(rows):
            spot = o // WIDTH * EIGHT + o % WIDTH
            chosen[q, spot:spot + 1, :] = jnp.where(odd == 1, line[rows - 1 - q:rows - q], line[q:q + 1])

    def window(block):
        return max(0, block * LANE - SUB), min(cols, (block + 1) * LANE + SUB)

    coef[...] = jnp.zeros_like(coef)
    late[...] = jnp.zeros_like(late)
    for block in range(blocks):
        begin, end = window(block)
        shape = (end - begin, LANE)
        shift = begin - block * LANE
        shift = shift + lax.broadcasted_iota(jnp.int32, shape, 0) - lax.broadcasted_iota(jnp.int32, shape, 1)
        for q in range(rows):
            for a in range(WIDTH):
                band = jnp.zeros(shape, jnp.float32)
                for b in range(WIDTH):
                    line = chosen[q, a * EIGHT + b:a * EIGHT + b + 1, block * LANE:(block + 1) * LANE]
                    band = jnp.where(shift == b - HALF, line, band)
                weight[block, q, a, 0:end - begin, :] = band

    def sides(block):
        ends = []
        if block > 0:
            ends.append(block * LANE - SUB)
        if block < blocks - 1:
            ends.append((block + 1) * LANE)
        return ends

    def set_edges(low):
        for block in range(blocks):
            for i in range(tiles):
                parts = []
                for end in sides(block):
                    if low > 0:
                        parts.append(jnp.zeros((low * SUB, LANE), edges.dtype))
                    for slot in range(low, span):
                        parts.append(turned[slot, i, end:end + SUB, :])
                used = len(sides(block)) * span * SUB
                if used < edges.shape[2]:
                    parts.append(jnp.zeros((edges.shape[2] - used, LANE), edges.dtype))
                edges[block, i * LANE:(i + 1) * LANE, :] = jnp.concatenate(parts, axis=0).T

    mate_all.wait_recv()
    if planes > 1:
        @pl.when(outer & has_far)
        def _():
            far_copy(0, 0, 1).start()
            send_rest()
    plane_rows[plane] = jnp.sum(powers[...], axis=0)
    if planes > 1:
        @pl.when(inner)
        def _():
            for d in range(planes - 2):
                meet_lane(d)
            for k in range(1, planes):
                plane_copy(k, plane).start()
            plane_all.wait_recv()
            whole_row[...] = jnp.sum(plane_rows[...], axis=0)
            whole_copy.start()

        @pl.when(outer)
        def _():
            whole_copy.wait_recv()
    else:
        whole_row[...] = plane_rows[0]
    power = whole_row[...]
    gain_row = lax.rsqrt(power * (1.0 / (total_rows * cols)) + 0.1)
    gains[...] = jnp.broadcast_to(gain_row, (LANE, long_dates)).T[0:half, :]
    tall = jnp.concatenate([gains[...], gains[...], jnp.zeros((long_depth - depth, LANE), jnp.float32)], axis=0)
    long_gain[...] = tall.T[0:8, :]

    def set_pair(q, block, real, imag):
        pairs[q, block, 0, 0:half, :] = real
        pairs[q, block, 1, 0:half, :] = imag
        pairs[q, block, 0, half:depth, :] = imag
        pairs[q, block, 1, half:depth, :] = -real

    for q in range(rows):
        for block in range(blocks):
            square = gains[...] * gains[...]
            tile = scene[HALF + q, block].astype(jnp.float32)
            set_pair(
                q, block, (tile[0:half] * square).astype(jnp.bfloat16), (tile[half:depth] * square).astype(jnp.bfloat16)
            )

    def project(q, block, slots, into_late=False):
        begin, end = window(block)
        size = end - begin
        main = block * LANE - begin
        left = jnp.concatenate(
            [jnp.concatenate([turned[slot, i, begin:end, :] for i in range(tiles)], axis=1) for slot in slots], axis=0
        )
        right = jnp.concatenate([pairs[q, block, 0], pairs[q, block, 1]], axis=1)
        proj = jnp.dot(left[:, 0:depth], right, preferred_element_type=jnp.float32)
        for i, slot in enumerate(slots):
            a = slot - q
            band = weight[block, q, a, 0:size, :]
            for c in range(2):
                part = (proj[i * size:(i + 1) * size, c * LANE:(c + 1) * LANE] * band).astype(jnp.bfloat16)
                if into_late:
                    late[q, block, c, begin:end, :] = part
                    continue
                coef[q, block, c, a * LANE:(a + 1) * LANE, :] = part[main:main + LANE]
                for k, side in enumerate(sides(block)):
                    spot = WIDTH * LANE + (k * span + slot) * SUB
                    coef[q, block, c, spot:spot + SUB, :] = part[side - begin:side - begin + SUB]

    def update(q, block, slots):
        left = jnp.concatenate([scene[s, block] for s in slots] + [edges[block, 0:depth, :]], axis=1)
        first = (slots[0] - q) * LANE
        right = jnp.concatenate([coef[q, block, 0, first:, :], coef[q, block, 1, first:, :]], axis=1)
        return jnp.dot(left, right, preferred_element_type=jnp.float32)

    def late_update(q, block, slot):
        left = jnp.concatenate([scene[slot, b] for b in range(blocks)], axis=1)
        right = jnp.concatenate([late[q, block, 0], late[q, block, 1]], axis=1)
        return jnp.dot(left, right, preferred_element_type=jnp.float32)

    def normalize(product):
        gain = gains[...]
        top, bottom = product[0:half], product[half:depth]
        real = (top[:, 0:LANE] - bottom[:, LANE:2 * LANE]) * gain
        imag = (top[:, LANE:2 * LANE] + bottom[:, 0:LANE]) * gain
        energy = jnp.sum(real * real + imag * imag, axis=0, keepdims=True)
        factor = lax.rsqrt(energy * (1.0 / ndate) + 0.001)
        return real * factor, imag * factor

    def first_step(q, block, product):
        real, imag = normalize(product)
        gain = gains[...]
        set_pair(q, block, (real * gain).astype(jnp.bfloat16), (imag * gain).astype(jnp.bfloat16))

    def last_steps(q):
        window_slots = list(range(q, q + WIDTH))
        for i in range(1, ITERS):
            for block in range(blocks):
                project(q, block, window_slots)
            products = [update(q, block, window_slots) for block in range(blocks)]
            for block in range(blocks):
                real, imag = normalize(products[block])
                if i < ITERS - 1:
                    gain = gains[...]
                    set_pair(q, block, (real * gain).astype(jnp.bfloat16), (imag * gain).astype(jnp.bfloat16))
                else:
                    vectors[q, block, 0:half, :] = real
                    vectors[q, block, half:depth, :] = imag

    def seen(q, slots):
        return [s for s in slots if q <= s < q + WIDTH]

    pl.when(has_near)(near_all.wait_recv)
    pl.when(has_far)(piece_copy.wait_recv)
    for t in range(HALF):
        turn(HALF + rows + t)
        pick(HALF + rows + t)
    set_edges(HALF)
    for q in range(rows):
        slots = seen(q, range(HALF, span))
        for block in range(blocks):
            project(q, block, slots)
        for block in range(blocks):
            total[q, block] = update(q, block, slots)

    def swap(x):
        lanes = lax.broadcasted_iota(jnp.int32, x.shape, 1)
        ahead = pltpu.roll(x, long_depth - half, 1)
        behind = pltpu.roll(x, half, 1)
        return jnp.where(lanes < half, -ahead, jnp.where(lanes < depth, behind, 0.0))

    def reference_vector(q):
        stack = jnp.concatenate([picks[q + a].astype(jnp.float32) for a in range(WIDTH)], axis=0)
        lanes = lax.broadcasted_iota(jnp.int32, (WIDTH * EIGHT, cols), 1)
        bands = jnp.sum(jnp.where(lanes == target_col, chosen[q], 0.0), axis=1, keepdims=True)
        middle = HALF * EIGHT + HALF
        center = stack[middle:middle + 1]
        gain = long_gain[0:1, :]
        vector = center * gain
        for _ in range(ITERS):
            vector = vector * gain
            proj_real = jnp.sum(stack * vector, axis=1, keepdims=True) * bands
            proj_imag = jnp.sum(stack * -swap(vector), axis=1, keepdims=True) * bands
            vector = jnp.sum(stack * proj_real, axis=0, keepdims=True)
            vector = vector + swap(jnp.sum(stack * proj_imag, axis=0, keepdims=True))
            vector = vector * gain
            energy = jnp.sum(vector * vector, axis=1, keepdims=True)
            vector = vector * lax.rsqrt(energy * (1.0 / ndate) + 0.001)
        return vector

    found = jnp.zeros((1, long_depth), jnp.float32)
    for q in range(rows):
        found = found + jnp.where(home == place(q), reference_vector(q), 0.0)
    refs[me] = found
    for k in range(1, n):
        ref_copy(k, me).start()

    for q in range(HALF, rows):
        for block in range(blocks):
            first_step(q, block, total[q, block])
        last_steps(q)
    for t in range(HALF):
        slot = HALF - 1 - t
        pl.when(has_far)(far_copy(t, 0, blocks).wait_recv)
        turn(slot)
        set_edges(slot)
        for q in range(min(slot, rows - 1), -1, -1):
            for block in range(blocks):
                project(q, block, [slot], into_late=True)
        if slot < rows:
            products = [late_update(slot, block, slot) for block in range(blocks)]
            for block in range(blocks):
                first_step(slot, block, total[slot, block] + products[block])
            last_steps(slot)
        for q in range(min(slot, rows) - 1, -1, -1):
            for block in range(blocks):
                total[q, block] += late_update(q, block, slot)

    ref_all.wait_recv()
    refvec = jnp.sum(refs[...], axis=0)
    refvec = jnp.broadcast_to(refvec, (LANE, long_depth)).T
    ref_real = refvec[0:half]
    ref_imag = refvec[half:depth]
    for q in range(rows):
        for block in range(blocks):
            real = vectors[q, block, 0:half, :]
            imag = vectors[q, block, half:depth, :]
            start = block * rows + place(q)
            out_ref[pl.ds(start, ndate, stride=stride), :] = (real * ref_real + imag * ref_imag)[0:ndate]
            start = start + ndate * stride
            out_ref[pl.ds(start, ndate, stride=stride), :] = (imag * ref_real - real * ref_imag)[0:ndate]

    pl.when(has_far)(far_all.wait_send)
    pl.when(has_far)(piece_copy.wait_send)
    pl.when(has_near)(near_all.wait_send)
    mate_all.wait_send()
    ref_all.wait_send()
    if planes > 1:
        @pl.when(inner)
        def _():
            plane_all.wait_send()
            whole_copy.wait_send()


def per_device(slc, mask, ref_index):
    parts, ndate, rows, cols = slc.shape
    n = lax.axis_size("row")
    group = GROUP if n % GROUP == 0 else n
    half = round_up(ndate, SUB)
    depth = 2 * half
    long_dates = round_up(half, LANE)
    long_depth = round_up(depth, LANE)
    blocks = cols // LANE
    span = rows + 2 * HALF
    lines = parts * ndate * blocks * rows
    margin = round_up(min(2, blocks - 1) * span * SUB, LANE)
    x = slc.reshape(parts, ndate, rows, blocks, LANE).transpose(0, 1, 3, 2, 4).reshape(lines, LANE)
    vmem = pl.BlockSpec(memory_space=pltpu.VMEM)
    anywhere = pl.BlockSpec(memory_space=pltpu.HBM)

    def body(*refs):
        kernel(n, ndate, *refs)

    out = pl.pallas_call(
        body,
        out_shape=jax.ShapeDtypeStruct((lines, LANE), jnp.float32),
        in_specs=[anywhere, anywhere, pl.BlockSpec(memory_space=pltpu.SMEM)],
        out_specs=vmem,
        scratch_shapes=[
            pltpu.VMEM((lines, LANE), jnp.bfloat16),
            pltpu.VMEM(mask.shape, jnp.int32),
            pltpu.VMEM((lines + (half - ndate) * blocks * rows, LANE), jnp.float32),
            pltpu.VMEM((span, blocks, depth, LANE), jnp.bfloat16),
            pltpu.VMEM((span, long_depth // LANE, cols, LANE), jnp.bfloat16),
            pltpu.VMEM((rows, WIDTH * EIGHT, cols), jnp.float32),
            pltpu.VMEM((span, EIGHT, long_depth), jnp.bfloat16),
            pltpu.VMEM((HALF, EIGHT, long_depth), jnp.bfloat16),
            pltpu.VMEM((blocks, rows, WIDTH, LANE + 2 * SUB, LANE), jnp.float32),
            pltpu.VMEM((rows, blocks, 2, depth, LANE), jnp.bfloat16),
            pltpu.VMEM((rows, blocks, 2, WIDTH * LANE + margin, LANE), jnp.bfloat16),
            pltpu.VMEM((rows, blocks, 2, cols, LANE), jnp.bfloat16),
            pltpu.VMEM((blocks, long_depth, margin), jnp.bfloat16),
            pltpu.VMEM((rows, blocks, depth, 2 * LANE), jnp.float32),
            pltpu.VMEM((rows, blocks, depth, LANE), jnp.float32),
            pltpu.VMEM((half, LANE), jnp.float32),
            pltpu.VMEM((8, long_depth), jnp.float32),
            pltpu.VMEM((long_depth, LANE), jnp.float32),
            pltpu.VMEM((group, 1, long_dates), jnp.float32),
            pltpu.VMEM((n // group, 1, long_dates), jnp.float32),
            pltpu.VMEM((1, long_dates), jnp.float32),
            pltpu.VMEM((n, 1, long_depth), jnp.float32),
            pltpu.SemaphoreType.DMA,
            pltpu.SemaphoreType.DMA,
            pltpu.SemaphoreType.REGULAR((2, max(1, n // group - 2))),
            pltpu.SemaphoreType.DMA((HALF + 1,)),
            pltpu.SemaphoreType.DMA((2,)),
            pltpu.SemaphoreType.DMA((2,)),
            pltpu.SemaphoreType.DMA((2,)),
            pltpu.SemaphoreType.DMA((2,)),
            pltpu.SemaphoreType.DMA((2,)),
            pltpu.SemaphoreType.DMA((2,)),
        ],
        compiler_params=pltpu.CompilerParams(collective_id=0, has_side_effects=True, vmem_limit_bytes=VMEM_LIMIT),
        name="link",
    )(pltpu.with_memory_space_constraint(x, pltpu.HBM), pltpu.with_memory_space_constraint(mask, pltpu.HBM), ref_index)

    def put(in_ref, out_ref, sem):
        copy = pltpu.make_async_copy(in_ref, out_ref, sem)
        copy.start()
        copy.wait()

    out = pl.pallas_call(
        put,
        out_shape=jax.ShapeDtypeStruct((lines, LANE), jnp.float32),
        in_specs=[vmem],
        out_specs=anywhere,
        scratch_shapes=[pltpu.SemaphoreType.DMA],
        compiler_params=pltpu.CompilerParams(vmem_limit_bytes=16 * 1024 * 1024),
        name="put",
    )(out)
    out = out.reshape(parts, ndate, blocks, rows, LANE).transpose(0, 1, 3, 2, 4)
    return out.reshape(parts, ndate, rows, cols)


def solution(mesh):
    placed = (P(None, None, ("grp", "row"), None), P(None, ("grp", "row"), None), P("grp"))
    return jax.shard_map(
        per_device,
        mesh=mesh,
        in_specs=placed,
        out_specs=P(None, None, ("grp", "row"), None),
        check_vma=False,
    )
```

```python
import jax
import jax.numpy as jnp
from jax import lax
from jax.experimental import pallas as pl
from jax.experimental.pallas import tpu as pltpu
from jax.sharding import PartitionSpec as P

HALF = 2
ITERS = 2
WIDTH = 2 * HALF + 1
LANE = 128
SUB = 16
EIGHT = 8
GROUP = 4
PUTS = 4
VMEM_LIMIT = 32000000
MESH = pl.DeviceIdType.MESH


def round_up(value, unit):
    return (value + unit - 1) // unit * unit


def kernel(
    n, ndate, x_hbm, mask_hbm, index_ref, out_ref,
    raw, mask_ref, wide, scene, turned, chosen, picks, pieces, weight, pairs, coef, late, edges, total, vectors, gains, long_gain, column, powers, plane_rows, whole_row, refs,
    load_sem, mask_sem, lane_sem, far_sem, near_sem, piece_sem, power_sem, plane_sem, whole_sem, ref_sem,
):
    _, rows, cols = mask_ref.shape
    span, blocks, depth, _ = scene.shape
    half = depth // 2
    tiles = turned.shape[1]
    long_depth = refs.shape[2]
    long_dates = powers.shape[2]
    total_rows = rows * n
    stride = blocks * rows
    me = lax.axis_index("row")
    odd = lax.rem(me, 2)
    near = me + 1 - 2 * odd
    far = me - 1 + 2 * odd
    has_near = near < n
    has_far = (far >= 0) & (far < n)
    first_row = me * rows

    def peer(k):
        return lax.rem(me + k, n)

    def place(q):
        return q + odd * (rows - 1 - 2 * q)

    part_rows = raw.shape[0] // 2

    def load(part):
        chunk = pl.ds(part * part_rows, part_rows)
        return pltpu.make_async_copy(x_hbm.at[chunk], raw.at[chunk], load_sem.at[part])

    for part in range(2):
        load(part).start()
    load_mask = pltpu.make_async_copy(mask_hbm, mask_ref, mask_sem)
    load_mask.start()
    group = GROUP if n % GROUP == 0 else n
    planes = n // group
    plane = me // group
    lane = lax.rem(me, group)
    has_up = plane < planes - 1
    has_down = plane > 0
    crosses = has_far & ((lane + 1 - 2 * (1 - odd) < 0) | (lane + 1 - 2 * (1 - odd) > group - 1))

    def signal(sem, target):
        pl.semaphore_signal(sem, inc=1, device_id={"row": target}, device_id_type=MESH)

    def signal_mates(sem):
        for k in range(1, group):
            signal(sem, plane * group + lax.rem(lane + k, group))

    barrier = pltpu.get_barrier_semaphore()
    pl.when(crosses)(lambda: signal(barrier, jnp.clip(far, 0, n - 1)))
    pl.when(has_up)(lambda: signal(barrier, jnp.minimum(me + group, n - 1)))
    pl.when(has_down)(lambda: signal(barrier, jnp.maximum(me - group, 0)))
    signal_mates(barrier)
    expected = group - 1 + has_up.astype(jnp.int32) + has_down.astype(jnp.int32) + crosses.astype(jnp.int32)

    def meet_lane(d):
        pl.when(has_up)(lambda: signal(lane_sem.at[0, d], jnp.minimum(me + group, n - 1)))
        pl.when(has_down)(lambda: signal(lane_sem.at[1, d], jnp.maximum(me - group, 0)))

        @pl.when(has_down)
        def _():
            pl.semaphore_wait(lane_sem.at[0, d], 1)

        @pl.when(has_up)
        def _():
            pl.semaphore_wait(lane_sem.at[1, d], 1)

    column[...] = jnp.zeros_like(column)

    sums = jnp.zeros((half, LANE), jnp.float32)
    dates = lax.broadcasted_iota(jnp.int32, (half, LANE), 0)
    for part in range(2):
        load(part).wait()
        chunk = slice(part * part_rows, (part + 1) * part_rows)
        wide[chunk, :] = raw[chunk, :].astype(jnp.float32)
        for q in range(rows):
            for block in range(blocks):
                start = part * part_rows + block * rows + place(q)
                piece = wide[pl.ds(start, half, stride=stride), :]
                piece = jnp.where(dates < ndate, piece, 0.0)
                scene[HALF + q, block, part * half:(part + 1) * half, :] = piece.astype(jnp.bfloat16)
                sums = sums + piece * piece
    column[0:half, :] = sums
    powers[lane] = jnp.sum(column[0:long_dates, :].T, axis=0, keepdims=True)

    target = index_ref[0]
    target_row = lax.div(target, cols) - first_row
    target_col = lax.rem(target, cols)
    base = jnp.clip(lax.div(target_col + SUB - HALF, SUB) - 1, 0, cols // SUB - 2)
    home = lax.broadcasted_iota(jnp.int32, (1, long_depth), 1) * 0 + target_row

    def turn(slot):
        for block in range(blocks):
            lines = slice(block * LANE, (block + 1) * LANE)
            for i in range(tiles):
                deep = slice(i * LANE, min((i + 1) * LANE, depth))
                tile = scene[slot, block, deep, :]
                if tile.shape[0] < LANE:
                    tile = jnp.concatenate([tile, jnp.zeros((LANE - tile.shape[0], LANE), tile.dtype)], axis=0)
                turned[slot, i, lines, :] = tile.T

    def pick(slot):
        group_of = lax.broadcasted_iota(jnp.int32, (SUB, LANE), 1) * 0 + base
        hits = [(group_of == k).astype(jnp.float32).astype(scene.dtype) for k in range(-1, cols // SUB)]
        strips = []
        for i in range(tiles):
            first = jnp.zeros((SUB, LANE), scene.dtype)
            second = first
            for k in range(cols // SUB):
                piece = turned[slot, i, k * SUB:(k + 1) * SUB, :]
                first = first + piece * hits[k + 1]
                second = second + piece * hits[k]
            strips.append(jnp.concatenate([first, second], axis=0))
        shape = (SUB, 2 * SUB)
        offset = lax.broadcasted_iota(jnp.int32, shape, 0)
        line = lax.broadcasted_iota(jnp.int32, shape, 1)
        hit = (line == target_col - HALF - base * SUB + offset) & (offset < WIDTH)
        left = hit.astype(jnp.float32).astype(scene.dtype)
        found = jnp.dot(left, jnp.concatenate(strips, axis=1), preferred_element_type=jnp.float32)
        picks[slot] = found[0:EIGHT].astype(scene.dtype)

    pl.semaphore_wait(barrier, expected)

    def mate_copy(k, rows_sent):
        return pltpu.make_async_remote_copy(
            src_ref=powers.at[rows_sent], dst_ref=powers.at[rows_sent],
            send_sem=power_sem.at[0], recv_sem=power_sem.at[1],
            device_id={"row": plane * group + lax.rem(lane + k, group)}, device_id_type=MESH,
        )

    def plane_copy(k, rows_sent):
        return pltpu.make_async_remote_copy(
            src_ref=plane_rows.at[rows_sent], dst_ref=plane_rows.at[rows_sent],
            send_sem=plane_sem.at[0], recv_sem=plane_sem.at[1],
            device_id={"row": lax.rem(plane + k, planes) * group + lane}, device_id_type=MESH,
        )

    def ref_copy(k, rows_sent):
        return pltpu.make_async_remote_copy(
            src_ref=refs.at[rows_sent], dst_ref=refs.at[rows_sent],
            send_sem=ref_sem.at[0], recv_sem=ref_sem.at[1],
            device_id={"row": peer(k)}, device_id_type=MESH,
        )

    mate_all = mate_copy(1, pl.ds(0, group - 1))
    ref_all = ref_copy(1, pl.ds(0, n - 1))
    if planes > 1:
        plane_all = plane_copy(1, pl.ds(0, planes - 1))

    inner = (lane > 0) & (lane < group - 1) if planes > 1 else lane >= 0
    outer = jnp.logical_not(inner)

    far_id = jnp.clip(far, 0, n - 1)
    near_id = jnp.clip(near, 0, n - 1)

    def far_copy(t, chunk=slice(None), deep=slice(None)):
        return pltpu.make_async_remote_copy(
            src_ref=scene.at[HALF + t, chunk, deep], dst_ref=scene.at[HALF - 1 - t, chunk, deep],
            send_sem=far_sem.at[HALF], recv_sem=far_sem.at[t],
            device_id={"row": far_id}, device_id_type=MESH,
        )

    far_first = far_copy(0, pl.ds(0, 1), pl.ds(0, half))

    def near_copy(t):
        return pltpu.make_async_remote_copy(
            src_ref=scene.at[HALF + rows - 1 - t], dst_ref=scene.at[HALF + rows + t],
            send_sem=near_sem.at[0], recv_sem=near_sem.at[1],
            device_id={"row": near_id}, device_id_type=MESH,
        )

    near_all = pltpu.make_async_remote_copy(
        src_ref=scene.at[pl.ds(HALF + rows - HALF, HALF)], dst_ref=scene.at[pl.ds(HALF + rows, HALF)],
        send_sem=near_sem.at[0], recv_sem=near_sem.at[1],
        device_id={"row": near_id}, device_id_type=MESH,
    )
    far_all = pltpu.make_async_remote_copy(
        src_ref=scene.at[pl.ds(HALF, HALF)], dst_ref=scene.at[pl.ds(0, HALF)],
        send_sem=far_sem.at[HALF], recv_sem=far_sem.at[0],
        device_id={"row": far_id}, device_id_type=MESH,
    )
    piece_copy = pltpu.make_async_remote_copy(
        src_ref=pieces, dst_ref=picks.at[pl.ds(0, HALF)],
        send_sem=piece_sem.at[0], recv_sem=piece_sem.at[1],
        device_id={"row": far_id}, device_id_type=MESH,
    )

    def send_rest():
        piece_copy.start()
        far_copy(0, pl.ds(0, 1), pl.ds(half, half)).start()
        far_copy(0, pl.ds(1, blocks - 1)).start()
        for t in range(1, HALF):
            far_copy(t).start()

    whole_copy = pltpu.make_async_remote_copy(
        src_ref=whole_row, dst_ref=whole_row, send_sem=whole_sem.at[0], recv_sem=whole_sem.at[1],
        device_id={"row": near_id}, device_id_type=MESH,
    )
    for k in range(1, group):
        mate_copy(k, lane).start()
    pl.when(inner & has_far)(far_first.start)
    for t in range(HALF):
        pl.when(has_near)(near_copy(t).start)
    for q in range(rows):
        turn(HALF + q)
        pick(HALF + q)
    for t in range(HALF):
        pieces[HALF - 1 - t] = picks[HALF + t]
    pl.when(inner & has_far)(send_rest)

    @pl.when(jnp.logical_not(has_far))
    def _():
        scene[0:HALF] = jnp.zeros((HALF, blocks, depth, LANE), scene.dtype)
        picks[0:HALF] = jnp.zeros((HALF, EIGHT, long_depth), scene.dtype)

    @pl.when(jnp.logical_not(has_near))
    def _():
        scene[HALF + rows:span] = jnp.zeros((HALF, blocks, depth, LANE), scene.dtype)

    load_mask.wait()
    row_ids = first_row + lax.broadcasted_iota(jnp.int32, (rows, cols), 0)
    col_ids = lax.broadcasted_iota(jnp.int32, (rows, cols), 1)
    count = jnp.zeros((rows, cols), jnp.float32)
    ones = []
    for a in range(WIDTH):
        step = a + odd * (WIDTH - 1 - 2 * a)
        for b in range(WIDTH):
            there = row_ids + (step - HALF)
            inside = (there >= 0) & (there < total_rows)
            inside = inside & (col_ids + (b - HALF) >= 0) & (col_ids + (b - HALF) < cols)
            if (a, b) != (HALF, HALF):
                inside = inside & (mask_ref[step * WIDTH + b] == 1)
            one = inside.astype(jnp.float32)
            ones.append(one)
            count = count + one
    inverse = 1.0 / (count * ndate)
    chosen[...] = jnp.zeros_like(chosen)
    for o in range(WIDTH * WIDTH):
        line = ones[o] * inverse
        for q in range(rows):
            spot = o // WIDTH * EIGHT + o % WIDTH
            chosen[q, spot:spot + 1, :] = jnp.where(odd == 1, line[rows - 1 - q:rows - q], line[q:q + 1])

    def window(block):
        return max(0, block * LANE - SUB), min(cols, (block + 1) * LANE + SUB)

    coef[...] = jnp.zeros_like(coef)
    late[...] = jnp.zeros_like(late)
    for block in range(blocks):
        begin, end = window(block)
        shape = (end - begin, LANE)
        shift = begin - block * LANE
        shift = shift + lax.broadcasted_iota(jnp.int32, shape, 0) - lax.broadcasted_iota(jnp.int32, shape, 1)
        for q in range(rows):
            for a in range(WIDTH):
                band = jnp.zeros(shape, jnp.float32)
                for b in range(WIDTH):
                    line = chosen[q, a * EIGHT + b:a * EIGHT + b + 1, block * LANE:(block + 1) * LANE]
                    band = jnp.where(shift == b - HALF, line, band)
                weight[block, q, a, 0:end - begin, :] = band

    def sides(block):
        ends = []
        if block > 0:
            ends.append(block * LANE - SUB)
        if block < blocks - 1:
            ends.append((block + 1) * LANE)
        return ends

    def set_edges(low):
        for block in range(blocks):
            for i in range(tiles):
                parts = []
                for end in sides(block):
                    if low > 0:
                        parts.append(jnp.zeros((low * SUB, LANE), edges.dtype))
                    for slot in range(low, span):
                        parts.append(turned[slot, i, end:end + SUB, :])
                used = len(sides(block)) * span * SUB
                if used < edges.shape[2]:
                    parts.append(jnp.zeros((edges.shape[2] - used, LANE), edges.dtype))
                edges[block, i * LANE:(i + 1) * LANE, :] = jnp.concatenate(parts, axis=0).T

    mate_all.wait_recv()
    if planes > 1:
        @pl.when(outer & has_far)
        def _():
            far_first.start()
            send_rest()
    plane_rows[plane] = jnp.sum(powers[...], axis=0)
    if planes > 1:
        @pl.when(inner)
        def _():
            for d in range(planes - 2):
                meet_lane(d)
            for k in range(1, planes):
                plane_copy(k, plane).start()
            plane_all.wait_recv()
            whole_row[...] = jnp.sum(plane_rows[...], axis=0)
            whole_copy.start()

        @pl.when(outer)
        def _():
            whole_copy.wait_recv()
    else:
        whole_row[...] = plane_rows[0]
    power = whole_row[...]
    gain_row = lax.rsqrt(power * (1.0 / (total_rows * cols)) + 0.1)
    gains[...] = jnp.broadcast_to(gain_row, (LANE, long_dates)).T[0:half, :]
    tall = jnp.concatenate([gains[...], gains[...], jnp.zeros((long_depth - depth, LANE), jnp.float32)], axis=0)
    long_gain[...] = tall.T[0:8, :]

    def set_pair(q, block, real, imag):
        pairs[q, block, 0, 0:half, :] = real
        pairs[q, block, 1, 0:half, :] = imag
        pairs[q, block, 0, half:depth, :] = imag
        pairs[q, block, 1, half:depth, :] = -real

    for q in range(rows):
        for block in range(blocks):
            square = gains[...] * gains[...]
            tile = scene[HALF + q, block].astype(jnp.float32)
            set_pair(
                q, block, (tile[0:half] * square).astype(jnp.bfloat16), (tile[half:depth] * square).astype(jnp.bfloat16)
            )

    def project(q, block, slots, into_late=False, factor=None):
        begin, end = window(block)
        size = end - begin
        main = block * LANE - begin
        left = jnp.concatenate(
            [jnp.concatenate([turned[slot, i, begin:end, :] for i in range(tiles)], axis=1) for slot in slots], axis=0
        )
        right = jnp.concatenate([pairs[q, block, 0], pairs[q, block, 1]], axis=1)
        proj = jnp.dot(left[:, 0:depth], right, preferred_element_type=jnp.float32)
        for i, slot in enumerate(slots):
            a = slot - q
            band = weight[block, q, a, 0:size, :]
            if factor is not None:
                band = band * factor
            for c in range(2):
                part = (proj[i * size:(i + 1) * size, c * LANE:(c + 1) * LANE] * band).astype(jnp.bfloat16)
                if into_late:
                    late[q, block, c, begin:end, :] = part
                    continue
                coef[q, block, c, a * LANE:(a + 1) * LANE, :] = part[main:main + LANE]
                for k, side in enumerate(sides(block)):
                    spot = WIDTH * LANE + (k * span + slot) * SUB
                    coef[q, block, c, spot:spot + SUB, :] = part[side - begin:side - begin + SUB]

    def update(q, block, slots):
        left = jnp.concatenate([scene[s, block] for s in slots] + [edges[block, 0:depth, :]], axis=1)
        first = (slots[0] - q) * LANE
        right = jnp.concatenate([coef[q, block, 0, first:, :], coef[q, block, 1, first:, :]], axis=1)
        return jnp.dot(left, right, preferred_element_type=jnp.float32)

    def late_update(q, block, slot):
        left = jnp.concatenate([scene[slot, b] for b in range(blocks)], axis=1)
        right = jnp.concatenate([late[q, block, 0], late[q, block, 1]], axis=1)
        return jnp.dot(left, right, preferred_element_type=jnp.float32)

    def combine(product):
        gain = gains[...]
        top, bottom = product[0:half], product[half:depth]
        real = (top[:, 0:LANE] - bottom[:, LANE:2 * LANE]) * gain
        imag = (top[:, LANE:2 * LANE] + bottom[:, 0:LANE]) * gain
        energy = jnp.sum(real * real + imag * imag, axis=0, keepdims=True)
        return real, imag, lax.rsqrt(energy * (1.0 / ndate) + 0.001)

    def first_step(q, block, product):
        real, imag, factor = combine(product)
        gain = gains[...]
        set_pair(q, block, (real * gain).astype(jnp.bfloat16), (imag * gain).astype(jnp.bfloat16))
        return factor

    def last_steps(q, factors):
        window_slots = list(range(q, q + WIDTH))
        for i in range(1, ITERS):
            for block in range(blocks):
                project(q, block, window_slots, factor=factors[block])
            products = [update(q, block, window_slots) for block in range(blocks)]
            if i < ITERS - 1:
                factors = [first_step(q, block, products[block]) for block in range(blocks)]
        for block in range(blocks):
            real, imag, factor = combine(products[block])
            vectors[q, block, 0:half, :] = real * factor
            vectors[q, block, half:depth, :] = imag * factor

    def seen(q, slots):
        return [s for s in slots if q <= s < q + WIDTH]

    pl.when(has_near)(near_all.wait_recv)
    pl.when(has_far)(piece_copy.wait_recv)
    for t in range(HALF):
        turn(HALF + rows + t)
        pick(HALF + rows + t)
    set_edges(HALF)
    for q in range(rows):
        slots = seen(q, range(HALF, span))
        for block in range(blocks):
            project(q, block, slots)
        for block in range(blocks):
            total[q, block] = update(q, block, slots)

    def swap(x):
        lanes = lax.broadcasted_iota(jnp.int32, x.shape, 1)
        ahead = pltpu.roll(x, long_depth - half, 1)
        behind = pltpu.roll(x, half, 1)
        return jnp.where(lanes < half, -ahead, jnp.where(lanes < depth, behind, 0.0))

    def reference_vector(q):
        stack = jnp.concatenate([picks[q + a].astype(jnp.float32) for a in range(WIDTH)], axis=0)
        lanes = lax.broadcasted_iota(jnp.int32, (WIDTH * EIGHT, cols), 1)
        bands = jnp.sum(jnp.where(lanes == target_col, chosen[q], 0.0), axis=1, keepdims=True)
        middle = HALF * EIGHT + HALF
        center = stack[middle:middle + 1]
        gain = long_gain[0:1, :]
        vector = center * gain
        for _ in range(ITERS):
            vector = vector * gain
            proj_real = jnp.sum(stack * vector, axis=1, keepdims=True) * bands
            proj_imag = jnp.sum(stack * -swap(vector), axis=1, keepdims=True) * bands
            vector = jnp.sum(stack * proj_real, axis=0, keepdims=True)
            vector = vector + swap(jnp.sum(stack * proj_imag, axis=0, keepdims=True))
            vector = vector * gain
            energy = jnp.sum(vector * vector, axis=1, keepdims=True)
            vector = vector * lax.rsqrt(energy * (1.0 / ndate) + 0.001)
        return vector

    found = jnp.zeros((1, long_depth), jnp.float32)
    for q in range(rows):
        found = found + jnp.where(home == place(q), reference_vector(q), 0.0)
    refs[me] = found
    for k in range(1, n):
        ref_copy(k, me).start()

    for q in range(HALF, rows):
        last_steps(q, [first_step(q, block, total[q, block]) for block in range(blocks)])
    for t in range(HALF):
        slot = HALF - 1 - t
        pl.when(has_far)(far_copy(t).wait_recv)
        turn(slot)
        set_edges(slot)
        for q in range(min(slot, rows - 1), -1, -1):
            for block in range(blocks):
                project(q, block, [slot], into_late=True)
        if slot < rows:
            products = [late_update(slot, block, slot) for block in range(blocks)]
            factors = [first_step(slot, block, total[slot, block] + products[block]) for block in range(blocks)]
            last_steps(slot, factors)
        for q in range(min(slot, rows) - 1, -1, -1):
            for block in range(blocks):
                total[q, block] += late_update(q, block, slot)

    ref_all.wait_recv()
    refvec = jnp.sum(refs[...], axis=0)
    refvec = jnp.broadcast_to(refvec, (LANE, long_depth)).T
    ref_real = refvec[0:half]
    ref_imag = refvec[half:depth]
    for q in range(rows):
        for block in range(blocks):
            real = vectors[q, block, 0:half, :]
            imag = vectors[q, block, half:depth, :]
            start = block * rows + place(q)
            out_ref[pl.ds(start, ndate, stride=stride), :] = (real * ref_real + imag * ref_imag)[0:ndate]
            start = start + ndate * stride
            out_ref[pl.ds(start, ndate, stride=stride), :] = (imag * ref_real - real * ref_imag)[0:ndate]

    pl.when(has_far)(far_all.wait_send)
    pl.when(has_far)(piece_copy.wait_send)
    pl.when(has_near)(near_all.wait_send)
    mate_all.wait_send()
    ref_all.wait_send()
    if planes > 1:
        @pl.when(inner)
        def _():
            plane_all.wait_send()
            whole_copy.wait_send()


def per_device(slc, mask, ref_index):
    parts, ndate, rows, cols = slc.shape
    n = lax.axis_size("row")
    group = GROUP if n % GROUP == 0 else n
    half = round_up(ndate, SUB)
    depth = 2 * half
    long_dates = round_up(half, LANE)
    long_depth = round_up(depth, LANE)
    blocks = cols // LANE
    span = rows + 2 * HALF
    lines = parts * ndate * blocks * rows
    margin = round_up(min(2, blocks - 1) * span * SUB, LANE)
    x = slc.reshape(parts, ndate, rows, blocks, LANE).transpose(0, 1, 3, 2, 4).reshape(lines, LANE)
    vmem = pl.BlockSpec(memory_space=pltpu.VMEM)
    anywhere = pl.BlockSpec(memory_space=pltpu.HBM)

    def body(*refs):
        kernel(n, ndate, *refs)

    out = pl.pallas_call(
        body,
        out_shape=jax.ShapeDtypeStruct((lines, LANE), jnp.float32),
        in_specs=[anywhere, anywhere, pl.BlockSpec(memory_space=pltpu.SMEM)],
        out_specs=vmem,
        scratch_shapes=[
            pltpu.VMEM((lines, LANE), jnp.bfloat16),
            pltpu.VMEM(mask.shape, jnp.int32),
            pltpu.VMEM((lines + (half - ndate) * blocks * rows, LANE), jnp.float32),
            pltpu.VMEM((span, blocks, depth, LANE), jnp.bfloat16),
            pltpu.VMEM((span, long_depth // LANE, cols, LANE), jnp.bfloat16),
            pltpu.VMEM((rows, WIDTH * EIGHT, cols), jnp.float32),
            pltpu.VMEM((span, EIGHT, long_depth), jnp.bfloat16),
            pltpu.VMEM((HALF, EIGHT, long_depth), jnp.bfloat16),
            pltpu.VMEM((blocks, rows, WIDTH, LANE + 2 * SUB, LANE), jnp.float32),
            pltpu.VMEM((rows, blocks, 2, depth, LANE), jnp.bfloat16),
            pltpu.VMEM((rows, blocks, 2, WIDTH * LANE + margin, LANE), jnp.bfloat16),
            pltpu.VMEM((rows, blocks, 2, cols, LANE), jnp.bfloat16),
            pltpu.VMEM((blocks, long_depth, margin), jnp.bfloat16),
            pltpu.VMEM((rows, blocks, depth, 2 * LANE), jnp.float32),
            pltpu.VMEM((rows, blocks, depth, LANE), jnp.float32),
            pltpu.VMEM((half, LANE), jnp.float32),
            pltpu.VMEM((8, long_depth), jnp.float32),
            pltpu.VMEM((long_depth, LANE), jnp.float32),
            pltpu.VMEM((group, 1, long_dates), jnp.float32),
            pltpu.VMEM((n // group, 1, long_dates), jnp.float32),
            pltpu.VMEM((1, long_dates), jnp.float32),
            pltpu.VMEM((n, 1, long_depth), jnp.float32),
            pltpu.SemaphoreType.DMA((2,)),
            pltpu.SemaphoreType.DMA,
            pltpu.SemaphoreType.REGULAR((2, max(1, n // group - 2))),
            pltpu.SemaphoreType.DMA((HALF + 1,)),
            pltpu.SemaphoreType.DMA((2,)),
            pltpu.SemaphoreType.DMA((2,)),
            pltpu.SemaphoreType.DMA((2,)),
            pltpu.SemaphoreType.DMA((2,)),
            pltpu.SemaphoreType.DMA((2,)),
            pltpu.SemaphoreType.DMA((2,)),
        ],
        compiler_params=pltpu.CompilerParams(collective_id=0, has_side_effects=True, vmem_limit_bytes=VMEM_LIMIT),
        name="link",
    )(pltpu.with_memory_space_constraint(x, pltpu.HBM), pltpu.with_memory_space_constraint(mask, pltpu.HBM), ref_index)

    def put(in_ref, out_ref, sem):
        size = lines // PUTS // EIGHT * EIGHT
        ends = [k * size for k in range(PUTS)] + [lines]
        copies = []
        for k in range(PUTS):
            chunk = pl.ds(ends[k], ends[k + 1] - ends[k])
            copies.append(pltpu.make_async_copy(in_ref.at[chunk], out_ref.at[chunk], sem.at[k]))
        for copy in copies:
            copy.start()
        for copy in copies:
            copy.wait()

    out = pl.pallas_call(
        put,
        out_shape=jax.ShapeDtypeStruct((lines, LANE), jnp.float32),
        in_specs=[vmem],
        out_specs=anywhere,
        scratch_shapes=[pltpu.SemaphoreType.DMA((PUTS,))],
        compiler_params=pltpu.CompilerParams(vmem_limit_bytes=16 * 1024 * 1024),
        name="put",
    )(out)
    out = out.reshape(parts, ndate, blocks, rows, LANE).transpose(0, 1, 3, 2, 4)
    return out.reshape(parts, ndate, rows, cols)


def solution(mesh):
    placed = (P(None, None, ("grp", "row"), None), P(None, ("grp", "row"), None), P("grp"))
    return jax.shard_map(
        per_device,
        mesh=mesh,
        in_specs=placed,
        out_specs=P(None, None, ("grp", "row"), None),
        check_vma=False,
    )
```

```python
import jax
import jax.numpy as jnp
from jax import lax
from jax.experimental import pallas as pl
from jax.experimental.pallas import tpu as pltpu
from jax.sharding import PartitionSpec as P

HALF = 2
ITERS = 2
WIDTH = 2 * HALF + 1
LANE = 128
SUB = 16
EIGHT = 8
GROUP = 4
PUTS = 3
VMEM_LIMIT = 32000000
MESH = pl.DeviceIdType.MESH


def round_up(value, unit):
    return (value + unit - 1) // unit * unit


def kernel(
    n, ndate, x_hbm, mask_hbm, index_hbm, vectors, columns,
    raw, mask_ref, index_ref, wide, scene, turned, chosen, picks, pieces, weight, pairs, coef, late, edges, total, gains, long_gain, column, powers, plane_rows, whole_row, refs,
    load_sem, mask_sem, index_sem, lane_sem, far_sem, near_sem, piece_sem, power_sem, plane_sem, whole_sem, ref_sem,
):
    _, rows, cols = mask_ref.shape
    span, blocks, depth, _ = scene.shape
    half = depth // 2
    tiles = turned.shape[1]
    long_depth = refs.shape[2]
    long_dates = powers.shape[2]
    total_rows = rows * n
    stride = blocks * rows
    me = lax.axis_index("row")
    odd = lax.rem(me, 2)
    near = me + 1 - 2 * odd
    far = me - 1 + 2 * odd
    has_near = near < n
    has_far = (far >= 0) & (far < n)
    first_row = me * rows

    def peer(k):
        return lax.rem(me + k, n)

    def place(q):
        return q + odd * (rows - 1 - 2 * q)

    part_rows = raw.shape[0] // 2

    def load(part):
        chunk = pl.ds(part * part_rows, part_rows)
        return pltpu.make_async_copy(x_hbm.at[chunk], raw.at[chunk], load_sem.at[part])

    for part in range(2):
        load(part).start()
    load_mask = pltpu.make_async_copy(mask_hbm, mask_ref, mask_sem)
    load_mask.start()
    load_index = pltpu.make_async_copy(index_hbm, index_ref, index_sem)
    load_index.start()
    group = GROUP if n % GROUP == 0 else n
    planes = n // group
    plane = me // group
    lane = lax.rem(me, group)
    has_up = plane < planes - 1
    has_down = plane > 0
    crosses = has_far & ((lane + 1 - 2 * (1 - odd) < 0) | (lane + 1 - 2 * (1 - odd) > group - 1))

    def signal(sem, target):
        pl.semaphore_signal(sem, inc=1, device_id={"row": target}, device_id_type=MESH)

    def signal_mates(sem):
        for k in range(1, group):
            signal(sem, plane * group + lax.rem(lane + k, group))

    barrier = pltpu.get_barrier_semaphore()
    pl.when(crosses)(lambda: signal(barrier, jnp.clip(far, 0, n - 1)))
    pl.when(has_up)(lambda: signal(barrier, jnp.minimum(me + group, n - 1)))
    pl.when(has_down)(lambda: signal(barrier, jnp.maximum(me - group, 0)))
    signal_mates(barrier)
    expected = group - 1 + has_up.astype(jnp.int32) + has_down.astype(jnp.int32) + crosses.astype(jnp.int32)

    def meet_lane(d):
        pl.when(has_up)(lambda: signal(lane_sem.at[0, d], jnp.minimum(me + group, n - 1)))
        pl.when(has_down)(lambda: signal(lane_sem.at[1, d], jnp.maximum(me - group, 0)))

        @pl.when(has_down)
        def _():
            pl.semaphore_wait(lane_sem.at[0, d], 1)

        @pl.when(has_up)
        def _():
            pl.semaphore_wait(lane_sem.at[1, d], 1)

    column[...] = jnp.zeros_like(column)

    sums = jnp.zeros((half, LANE), jnp.float32)
    dates = lax.broadcasted_iota(jnp.int32, (half, LANE), 0)
    for part in range(2):
        load(part).wait()
        chunk = slice(part * part_rows, (part + 1) * part_rows)
        wide[chunk, :] = raw[chunk, :].astype(jnp.float32)
        for q in range(rows):
            for block in range(blocks):
                start = part * part_rows + block * rows + place(q)
                piece = wide[pl.ds(start, half, stride=stride), :]
                piece = jnp.where(dates < ndate, piece, 0.0)
                scene[HALF + q, block, part * half:(part + 1) * half, :] = piece.astype(jnp.bfloat16)
                sums = sums + piece * piece
    column[0:half, :] = sums
    powers[lane] = jnp.sum(column[0:long_dates, :].T, axis=0, keepdims=True)

    load_index.wait()
    target = index_ref[0]
    target_row = lax.div(target, cols) - first_row
    target_col = lax.rem(target, cols)
    base = jnp.clip(lax.div(target_col + SUB - HALF, SUB) - 1, 0, cols // SUB - 2)
    home = lax.broadcasted_iota(jnp.int32, (1, long_depth), 1) * 0 + target_row

    def turn(slot):
        for block in range(blocks):
            lines = slice(block * LANE, (block + 1) * LANE)
            for i in range(tiles):
                deep = slice(i * LANE, min((i + 1) * LANE, depth))
                tile = scene[slot, block, deep, :]
                if tile.shape[0] < LANE:
                    tile = jnp.concatenate([tile, jnp.zeros((LANE - tile.shape[0], LANE), tile.dtype)], axis=0)
                turned[slot, i, lines, :] = tile.T

    def pick(slot):
        group_of = lax.broadcasted_iota(jnp.int32, (SUB, LANE), 1) * 0 + base
        hits = [(group_of == k).astype(jnp.float32).astype(scene.dtype) for k in range(-1, cols // SUB)]
        strips = []
        for i in range(tiles):
            first = jnp.zeros((SUB, LANE), scene.dtype)
            second = first
            for k in range(cols // SUB):
                piece = turned[slot, i, k * SUB:(k + 1) * SUB, :]
                first = first + piece * hits[k + 1]
                second = second + piece * hits[k]
            strips.append(jnp.concatenate([first, second], axis=0))
        shape = (SUB, 2 * SUB)
        offset = lax.broadcasted_iota(jnp.int32, shape, 0)
        line = lax.broadcasted_iota(jnp.int32, shape, 1)
        hit = (line == target_col - HALF - base * SUB + offset) & (offset < WIDTH)
        left = hit.astype(jnp.float32).astype(scene.dtype)
        found = jnp.dot(left, jnp.concatenate(strips, axis=1), preferred_element_type=jnp.float32)
        picks[slot] = found[0:EIGHT].astype(scene.dtype)

    pl.semaphore_wait(barrier, expected)

    def mate_copy(k, rows_sent):
        return pltpu.make_async_remote_copy(
            src_ref=powers.at[rows_sent], dst_ref=powers.at[rows_sent],
            send_sem=power_sem.at[0], recv_sem=power_sem.at[1],
            device_id={"row": plane * group + lax.rem(lane + k, group)}, device_id_type=MESH,
        )

    def plane_copy(k, rows_sent):
        return pltpu.make_async_remote_copy(
            src_ref=plane_rows.at[rows_sent], dst_ref=plane_rows.at[rows_sent],
            send_sem=plane_sem.at[0], recv_sem=plane_sem.at[1],
            device_id={"row": lax.rem(plane + k, planes) * group + lane}, device_id_type=MESH,
        )

    def ref_copy(k, rows_sent):
        return pltpu.make_async_remote_copy(
            src_ref=refs.at[rows_sent], dst_ref=refs.at[rows_sent],
            send_sem=ref_sem.at[0], recv_sem=ref_sem.at[1],
            device_id={"row": peer(k)}, device_id_type=MESH,
        )

    mate_all = mate_copy(1, pl.ds(0, group - 1))
    ref_all = ref_copy(1, pl.ds(0, n - 1))
    if planes > 1:
        plane_all = plane_copy(1, pl.ds(0, planes - 1))

    inner = (lane > 0) & (lane < group - 1) if planes > 1 else lane >= 0
    outer = jnp.logical_not(inner)

    far_id = jnp.clip(far, 0, n - 1)
    near_id = jnp.clip(near, 0, n - 1)

    def far_copy(t, chunk=slice(None), deep=slice(None)):
        return pltpu.make_async_remote_copy(
            src_ref=scene.at[HALF + t, chunk, deep], dst_ref=scene.at[HALF - 1 - t, chunk, deep],
            send_sem=far_sem.at[HALF], recv_sem=far_sem.at[t],
            device_id={"row": far_id}, device_id_type=MESH,
        )

    far_first = far_copy(0, pl.ds(0, 1), pl.ds(0, half))

    def near_copy(t):
        return pltpu.make_async_remote_copy(
            src_ref=scene.at[HALF + rows - 1 - t], dst_ref=scene.at[HALF + rows + t],
            send_sem=near_sem.at[0], recv_sem=near_sem.at[1],
            device_id={"row": near_id}, device_id_type=MESH,
        )

    near_all = pltpu.make_async_remote_copy(
        src_ref=scene.at[pl.ds(HALF + rows - HALF, HALF)], dst_ref=scene.at[pl.ds(HALF + rows, HALF)],
        send_sem=near_sem.at[0], recv_sem=near_sem.at[1],
        device_id={"row": near_id}, device_id_type=MESH,
    )
    far_all = pltpu.make_async_remote_copy(
        src_ref=scene.at[pl.ds(HALF, HALF)], dst_ref=scene.at[pl.ds(0, HALF)],
        send_sem=far_sem.at[HALF], recv_sem=far_sem.at[0],
        device_id={"row": far_id}, device_id_type=MESH,
    )
    piece_copy = pltpu.make_async_remote_copy(
        src_ref=pieces, dst_ref=picks.at[pl.ds(0, HALF)],
        send_sem=piece_sem.at[0], recv_sem=piece_sem.at[1],
        device_id={"row": far_id}, device_id_type=MESH,
    )

    def send_rest():
        piece_copy.start()
        far_copy(0, pl.ds(0, 1), pl.ds(half, half)).start()
        far_copy(0, pl.ds(1, blocks - 1)).start()
        for t in range(1, HALF):
            far_copy(t).start()

    whole_copy = pltpu.make_async_remote_copy(
        src_ref=whole_row, dst_ref=whole_row, send_sem=whole_sem.at[0], recv_sem=whole_sem.at[1],
        device_id={"row": near_id}, device_id_type=MESH,
    )
    for k in range(1, group):
        mate_copy(k, lane).start()
    pl.when(inner & has_far)(far_first.start)
    for q in range(rows):
        turn(HALF + q)
        pick(HALF + q)
    for t in range(HALF):
        pieces[HALF - 1 - t] = picks[HALF + t]
    pl.when(inner & has_far)(send_rest)

    @pl.when(jnp.logical_not(has_far))
    def _():
        scene[0:HALF] = jnp.zeros((HALF, blocks, depth, LANE), scene.dtype)
        picks[0:HALF] = jnp.zeros((HALF, EIGHT, long_depth), scene.dtype)

    @pl.when(jnp.logical_not(has_near))
    def _():
        scene[HALF + rows:span] = jnp.zeros((HALF, blocks, depth, LANE), scene.dtype)

    load_mask.wait()
    row_ids = first_row + lax.broadcasted_iota(jnp.int32, (rows, cols), 0)
    col_ids = lax.broadcasted_iota(jnp.int32, (rows, cols), 1)
    count = jnp.zeros((rows, cols), jnp.float32)
    ones = []
    for a in range(WIDTH):
        step = a + odd * (WIDTH - 1 - 2 * a)
        for b in range(WIDTH):
            there = row_ids + (step - HALF)
            inside = (there >= 0) & (there < total_rows)
            inside = inside & (col_ids + (b - HALF) >= 0) & (col_ids + (b - HALF) < cols)
            if (a, b) != (HALF, HALF):
                inside = inside & (mask_ref[step * WIDTH + b] == 1)
            one = inside.astype(jnp.float32)
            ones.append(one)
            count = count + one
    inverse = 1.0 / (count * ndate)
    chosen[...] = jnp.zeros_like(chosen)
    for o in range(WIDTH * WIDTH):
        line = ones[o] * inverse
        for q in range(rows):
            spot = o // WIDTH * EIGHT + o % WIDTH
            chosen[q, spot:spot + 1, :] = jnp.where(odd == 1, line[rows - 1 - q:rows - q], line[q:q + 1])

    def window(block):
        return max(0, block * LANE - SUB), min(cols, (block + 1) * LANE + SUB)

    coef[...] = jnp.zeros_like(coef)
    late[...] = jnp.zeros_like(late)
    for block in range(blocks):
        begin, end = window(block)
        shape = (end - begin, LANE)
        shift = begin - block * LANE
        shift = shift + lax.broadcasted_iota(jnp.int32, shape, 0) - lax.broadcasted_iota(jnp.int32, shape, 1)
        for q in range(rows):
            for a in range(WIDTH):
                band = jnp.zeros(shape, jnp.float32)
                for b in range(WIDTH):
                    line = chosen[q, a * EIGHT + b:a * EIGHT + b + 1, block * LANE:(block + 1) * LANE]
                    band = jnp.where(shift == b - HALF, line, band)
                weight[block, q, a, 0:end - begin, :] = band

    def sides(block):
        ends = []
        if block > 0:
            ends.append(block * LANE - SUB)
        if block < blocks - 1:
            ends.append((block + 1) * LANE)
        return ends

    def set_edges(low):
        for block in range(blocks):
            for i in range(tiles):
                parts = []
                for end in sides(block):
                    if low > 0:
                        parts.append(jnp.zeros((low * SUB, LANE), edges.dtype))
                    for slot in range(low, span):
                        parts.append(turned[slot, i, end:end + SUB, :])
                used = len(sides(block)) * span * SUB
                if used < edges.shape[2]:
                    parts.append(jnp.zeros((edges.shape[2] - used, LANE), edges.dtype))
                edges[block, i * LANE:(i + 1) * LANE, :] = jnp.concatenate(parts, axis=0).T

    for t in range(HALF):
        pl.when(has_near)(near_copy(t).start)
    mate_all.wait_recv()
    if planes > 1:
        @pl.when(outer & has_far)
        def _():
            far_first.start()
            send_rest()
    plane_rows[plane] = jnp.sum(powers[...], axis=0)
    if planes > 1:
        @pl.when(inner)
        def _():
            for d in range(planes - 2):
                meet_lane(d)
            for k in range(1, planes):
                plane_copy(k, plane).start()
            plane_all.wait_recv()
            whole_row[...] = jnp.sum(plane_rows[...], axis=0)
            whole_copy.start()

        @pl.when(outer)
        def _():
            whole_copy.wait_recv()
    else:
        whole_row[...] = plane_rows[0]
    power = whole_row[...]
    gain_row = lax.rsqrt(power * (1.0 / (total_rows * cols)) + 0.1)
    gains[...] = jnp.broadcast_to(gain_row, (LANE, long_dates)).T[0:half, :]
    tall = jnp.concatenate([gains[...], gains[...], jnp.zeros((long_depth - depth, LANE), jnp.float32)], axis=0)
    long_gain[...] = tall.T[0:8, :]

    def set_pair(q, block, real, imag):
        pairs[q, block, 0, 0:half, :] = real
        pairs[q, block, 1, 0:half, :] = imag
        pairs[q, block, 0, half:depth, :] = imag
        pairs[q, block, 1, half:depth, :] = -real

    for q in range(rows):
        for block in range(blocks):
            square = gains[...] * gains[...]
            tile = scene[HALF + q, block].astype(jnp.float32)
            set_pair(
                q, block, (tile[0:half] * square).astype(jnp.bfloat16), (tile[half:depth] * square).astype(jnp.bfloat16)
            )

    def project(q, block, slots, into_late=False, factor=None):
        begin, end = window(block)
        size = end - begin
        main = block * LANE - begin
        left = jnp.concatenate(
            [jnp.concatenate([turned[slot, i, begin:end, :] for i in range(tiles)], axis=1) for slot in slots], axis=0
        )
        right = jnp.concatenate([pairs[q, block, 0], pairs[q, block, 1]], axis=1)
        proj = jnp.dot(left[:, 0:depth], right, preferred_element_type=jnp.float32)
        for i, slot in enumerate(slots):
            a = slot - q
            band = weight[block, q, a, 0:size, :]
            if factor is not None:
                band = band * factor
            for c in range(2):
                part = (proj[i * size:(i + 1) * size, c * LANE:(c + 1) * LANE] * band).astype(jnp.bfloat16)
                if into_late:
                    late[q, block, c, begin:end, :] = part
                    continue
                coef[q, block, c, a * LANE:(a + 1) * LANE, :] = part[main:main + LANE]
                for k, side in enumerate(sides(block)):
                    spot = WIDTH * LANE + (k * span + slot) * SUB
                    coef[q, block, c, spot:spot + SUB, :] = part[side - begin:side - begin + SUB]

    def update(q, block, slots):
        left = jnp.concatenate([scene[s, block] for s in slots] + [edges[block, 0:depth, :]], axis=1)
        first = (slots[0] - q) * LANE
        right = jnp.concatenate([coef[q, block, 0, first:, :], coef[q, block, 1, first:, :]], axis=1)
        return jnp.dot(left, right, preferred_element_type=jnp.float32)

    def late_update(q, block, slot):
        left = jnp.concatenate([scene[slot, b] for b in range(blocks)], axis=1)
        right = jnp.concatenate([late[q, block, 0], late[q, block, 1]], axis=1)
        return jnp.dot(left, right, preferred_element_type=jnp.float32)

    def combine(product):
        gain = gains[...]
        top, bottom = product[0:half], product[half:depth]
        real = (top[:, 0:LANE] - bottom[:, LANE:2 * LANE]) * gain
        imag = (top[:, LANE:2 * LANE] + bottom[:, 0:LANE]) * gain
        energy = jnp.sum(real * real + imag * imag, axis=0, keepdims=True)
        return real, imag, lax.rsqrt(energy * (1.0 / ndate) + 0.001)

    def first_step(q, block, product):
        real, imag, factor = combine(product)
        gain = gains[...]
        set_pair(q, block, (real * gain).astype(jnp.bfloat16), (imag * gain).astype(jnp.bfloat16))
        return factor

    def last_steps(q, factors):
        window_slots = list(range(q, q + WIDTH))
        for i in range(1, ITERS):
            for block in range(blocks):
                project(q, block, window_slots, factor=factors[block])
            products = [update(q, block, window_slots) for block in range(blocks)]
            if i < ITERS - 1:
                factors = [first_step(q, block, products[block]) for block in range(blocks)]
        for block in range(blocks):
            real, imag, factor = combine(products[block])
            vectors[place(q), block, 0:half, :] = real * factor
            vectors[place(q), block, half:depth, :] = imag * factor

    def seen(q, slots):
        return [s for s in slots if q <= s < q + WIDTH]

    pl.when(has_near)(near_all.wait_recv)
    pl.when(has_far)(piece_copy.wait_recv)
    for t in range(HALF):
        turn(HALF + rows + t)
        pick(HALF + rows + t)
    set_edges(HALF)
    for q in range(rows):
        slots = seen(q, range(HALF, span))
        for block in range(blocks):
            project(q, block, slots)
        for block in range(blocks):
            total[q, block] = update(q, block, slots)

    def swap(x):
        lanes = lax.broadcasted_iota(jnp.int32, x.shape, 1)
        ahead = pltpu.roll(x, long_depth - half, 1)
        behind = pltpu.roll(x, half, 1)
        return jnp.where(lanes < half, -ahead, jnp.where(lanes < depth, behind, 0.0))

    def reference_vector(q):
        stack = jnp.concatenate([picks[q + a].astype(jnp.float32) for a in range(WIDTH)], axis=0)
        lanes = lax.broadcasted_iota(jnp.int32, (WIDTH * EIGHT, cols), 1)
        bands = jnp.sum(jnp.where(lanes == target_col, chosen[q], 0.0), axis=1, keepdims=True)
        middle = HALF * EIGHT + HALF
        center = stack[middle:middle + 1]
        gain = long_gain[0:1, :]
        vector = center * gain
        for _ in range(ITERS):
            vector = vector * gain
            proj_real = jnp.sum(stack * vector, axis=1, keepdims=True) * bands
            proj_imag = jnp.sum(stack * -swap(vector), axis=1, keepdims=True) * bands
            vector = jnp.sum(stack * proj_real, axis=0, keepdims=True)
            vector = vector + swap(jnp.sum(stack * proj_imag, axis=0, keepdims=True))
            vector = vector * gain
            energy = jnp.sum(vector * vector, axis=1, keepdims=True)
            vector = vector * lax.rsqrt(energy * (1.0 / ndate) + 0.001)
        return vector

    found = jnp.zeros((1, long_depth), jnp.float32)
    for q in range(rows):
        found = found + jnp.where(home == place(q), reference_vector(q), 0.0)
    refs[me] = found
    for k in range(1, n):
        ref_copy(k, me).start()

    for q in range(HALF, rows):
        last_steps(q, [first_step(q, block, total[q, block]) for block in range(blocks)])
    for t in range(HALF):
        slot = HALF - 1 - t
        pl.when(has_far)(far_copy(t).wait_recv)
        turn(slot)
        set_edges(slot)
        for q in range(min(slot, rows - 1), -1, -1):
            for block in range(blocks):
                project(q, block, [slot], into_late=True)
        if slot < rows:
            products = [late_update(slot, block, slot) for block in range(blocks)]
            factors = [first_step(slot, block, total[slot, block] + products[block]) for block in range(blocks)]
            last_steps(slot, factors)
        for q in range(min(slot, rows) - 1, -1, -1):
            for block in range(blocks):
                total[q, block] += late_update(q, block, slot)

    ref_all.wait_recv()
    refvec = jnp.sum(refs[...], axis=0)
    columns[...] = jnp.broadcast_to(refvec, (LANE, long_depth)).T[0:depth]

    pl.when(has_far)(far_all.wait_send)
    pl.when(has_far)(piece_copy.wait_send)
    pl.when(has_near)(near_all.wait_send)
    mate_all.wait_send()
    ref_all.wait_send()
    if planes > 1:
        @pl.when(inner)
        def _():
            plane_all.wait_send()
            whole_copy.wait_send()


def per_device(slc, mask, ref_index):
    parts, ndate, rows, cols = slc.shape
    n = lax.axis_size("row")
    group = GROUP if n % GROUP == 0 else n
    half = round_up(ndate, SUB)
    depth = 2 * half
    long_dates = round_up(half, LANE)
    long_depth = round_up(depth, LANE)
    blocks = cols // LANE
    span = rows + 2 * HALF
    lines = parts * ndate * blocks * rows
    margin = round_up(min(2, blocks - 1) * span * SUB, LANE)
    x = slc.reshape(parts, ndate, rows, blocks, LANE).transpose(0, 1, 3, 2, 4).reshape(lines, LANE)
    vmem = pl.BlockSpec(memory_space=pltpu.VMEM)
    anywhere = pl.BlockSpec(memory_space=pltpu.HBM)

    def body(*refs):
        kernel(n, ndate, *refs)

    def in_hbm(array):
        return pltpu.with_memory_space_constraint(array, pltpu.HBM)

    vectors, columns = pl.pallas_call(
        body,
        out_shape=(
            jax.ShapeDtypeStruct((rows, blocks, depth, LANE), jnp.float32),
            jax.ShapeDtypeStruct((depth, LANE), jnp.float32),
        ),
        in_specs=[anywhere, anywhere, anywhere],
        out_specs=(vmem, vmem),
        scratch_shapes=[
            pltpu.VMEM((lines, LANE), jnp.bfloat16),
            pltpu.VMEM(mask.shape, jnp.int32),
            pltpu.SMEM(ref_index.shape, jnp.int32),
            pltpu.VMEM((lines + (half - ndate) * blocks * rows, LANE), jnp.float32),
            pltpu.VMEM((span, blocks, depth, LANE), jnp.bfloat16),
            pltpu.VMEM((span, long_depth // LANE, cols, LANE), jnp.bfloat16),
            pltpu.VMEM((rows, WIDTH * EIGHT, cols), jnp.float32),
            pltpu.VMEM((span, EIGHT, long_depth), jnp.bfloat16),
            pltpu.VMEM((HALF, EIGHT, long_depth), jnp.bfloat16),
            pltpu.VMEM((blocks, rows, WIDTH, LANE + 2 * SUB, LANE), jnp.float32),
            pltpu.VMEM((rows, blocks, 2, depth, LANE), jnp.bfloat16),
            pltpu.VMEM((rows, blocks, 2, WIDTH * LANE + margin, LANE), jnp.bfloat16),
            pltpu.VMEM((rows, blocks, 2, cols, LANE), jnp.bfloat16),
            pltpu.VMEM((blocks, long_depth, margin), jnp.bfloat16),
            pltpu.VMEM((rows, blocks, depth, 2 * LANE), jnp.float32),
            pltpu.VMEM((half, LANE), jnp.float32),
            pltpu.VMEM((8, long_depth), jnp.float32),
            pltpu.VMEM((long_depth, LANE), jnp.float32),
            pltpu.VMEM((group, 1, long_dates), jnp.float32),
            pltpu.VMEM((n // group, 1, long_dates), jnp.float32),
            pltpu.VMEM((1, long_dates), jnp.float32),
            pltpu.VMEM((n, 1, long_depth), jnp.float32),
            pltpu.SemaphoreType.DMA((2,)),
            pltpu.SemaphoreType.DMA,
            pltpu.SemaphoreType.DMA,
            pltpu.SemaphoreType.REGULAR((2, max(1, n // group - 2))),
            pltpu.SemaphoreType.DMA((HALF + 1,)),
            pltpu.SemaphoreType.DMA((2,)),
            pltpu.SemaphoreType.DMA((2,)),
            pltpu.SemaphoreType.DMA((2,)),
            pltpu.SemaphoreType.DMA((2,)),
            pltpu.SemaphoreType.DMA((2,)),
            pltpu.SemaphoreType.DMA((2,)),
        ],
        compiler_params=pltpu.CompilerParams(collective_id=0, has_side_effects=True, vmem_limit_bytes=VMEM_LIMIT),
        name="link",
    )(in_hbm(x), in_hbm(mask), ref_index)

    def put(vectors, columns, out_ref, stage, sem):
        size = round_up(ndate // PUTS, EIGHT)
        copies = []
        for k in range(PUTS):
            first, last = k * size, min((k + 1) * size, ndate)
            low, high = slice(first, last), slice(half + first, half + last)
            ref_real, ref_imag = columns[low, :], columns[high, :]
            for block in range(blocks):
                for row in range(rows):
                    real, imag = vectors[row, block, low, :], vectors[row, block, high, :]
                    start = (first * blocks + block) * rows + row
                    stride = blocks * rows
                    stage[pl.ds(start, last - first, stride=stride), :] = real * ref_real + imag * ref_imag
                    start = start + ndate * stride
                    stage[pl.ds(start, last - first, stride=stride), :] = imag * ref_real - real * ref_imag
            for part in range(parts):
                chunk = pl.ds((part * ndate + first) * blocks * rows, (last - first) * blocks * rows)
                copy = pltpu.make_async_copy(stage.at[chunk], out_ref.at[chunk], sem.at[k, part])
                copy.start()
                copies.append(copy)
        for copy in copies:
            copy.wait()

    out = pl.pallas_call(
        put,
        out_shape=jax.ShapeDtypeStruct((lines, LANE), jnp.float32),
        in_specs=[vmem, vmem],
        out_specs=anywhere,
        scratch_shapes=[pltpu.VMEM((lines, LANE), jnp.float32), pltpu.SemaphoreType.DMA((PUTS, parts))],
        compiler_params=pltpu.CompilerParams(vmem_limit_bytes=16 * 1024 * 1024),
        name="put",
    )(vectors, columns)
    out = out.reshape(parts, ndate, blocks, rows, LANE).transpose(0, 1, 3, 2, 4)
    return out.reshape(parts, ndate, rows, cols)


def solution(mesh):
    placed = (P(None, None, ("grp", "row"), None), P(None, ("grp", "row"), None), P("grp"))
    return jax.shard_map(
        per_device,
        mesh=mesh,
        in_specs=placed,
        out_specs=P(None, None, ("grp", "row"), None),
        check_vma=False,
    )
```

```python
import jax
import jax.numpy as jnp
from jax import lax
from jax.experimental import pallas as pl
from jax.experimental.pallas import tpu as pltpu
from jax.sharding import PartitionSpec as P

HALF = 2
ITERS = 2
WIDTH = 2 * HALF + 1
LANE = 128
SUB = 16
EIGHT = 8
GROUP = 4
PUTS = 3
VMEM_LIMIT = 32000000
MESH = pl.DeviceIdType.MESH


def round_up(value, unit):
    return (value + unit - 1) // unit * unit


def kernel(
    n, ndate, x_hbm, mask_hbm, index_hbm, vectors, columns,
    raw, mask_ref, index_ref, wide, scene, turned, chosen, picks, pieces, weight, pairs, coef, late, edges, total, gains, long_gain, column, powers, plane_rows, refs,
    load_sem, mask_sem, index_sem, meet_sem, lane_sem, far_sem, near_sem, piece_sem, power_sem, plane_sem, ref_sem,
):
    _, rows, cols = mask_ref.shape
    span, blocks, depth, _ = scene.shape
    half = depth // 2
    tiles = turned.shape[1]
    long_depth = refs.shape[2]
    long_dates = powers.shape[2]
    total_rows = rows * n
    stride = blocks * rows
    me = lax.axis_index("row")
    odd = lax.rem(me, 2)
    near = me + 1 - 2 * odd
    far = me - 1 + 2 * odd
    has_near = near < n
    has_far = (far >= 0) & (far < n)
    first_row = me * rows

    def peer(k):
        return lax.rem(me + k, n)

    def place(q):
        return q + odd * (rows - 1 - 2 * q)

    part_rows = raw.shape[0] // 2

    def load(part):
        chunk = pl.ds(part * part_rows, part_rows)
        return pltpu.make_async_copy(x_hbm.at[chunk], raw.at[chunk], load_sem.at[part])

    for part in range(2):
        load(part).start()
    load_mask = pltpu.make_async_copy(mask_hbm, mask_ref, mask_sem)
    load_mask.start()
    load_index = pltpu.make_async_copy(index_hbm, index_ref, index_sem)
    load_index.start()
    group = GROUP if n % GROUP == 0 else n
    planes = n // group
    plane = me // group
    lane = lax.rem(me, group)
    has_up = plane < planes - 1
    has_down = plane > 0
    crosses = has_far & ((lane + 1 - 2 * (1 - odd) < 0) | (lane + 1 - 2 * (1 - odd) > group - 1))

    inner = (lane > 0) & (lane < group - 1) if planes > 1 else lane >= 0
    outer = jnp.logical_not(inner)

    def signal(sem, target):
        pl.semaphore_signal(sem, inc=1, device_id={"row": target}, device_id_type=MESH)

    def signal_mates(sem):
        for k in range(1, group):
            signal(sem, plane * group + lax.rem(lane + k, group))

    barrier = pltpu.get_barrier_semaphore()
    pl.when(crosses)(lambda: signal(barrier, jnp.clip(far, 0, n - 1)))
    hub = me + inner.astype(jnp.int32) * (near - me)
    pl.when(has_up)(lambda: signal(barrier, jnp.minimum(hub + group, n - 1)))
    pl.when(has_down)(lambda: signal(barrier, jnp.maximum(hub - group, 0)))
    signal_mates(barrier)
    others = 2 * has_up.astype(jnp.int32) + 2 * has_down.astype(jnp.int32) + crosses.astype(jnp.int32)
    expected = group - 1 + outer.astype(jnp.int32) * others

    def meet_lane(d):
        pl.when(has_up)(lambda: signal(lane_sem.at[0, d], jnp.minimum(me + group, n - 1)))
        pl.when(has_down)(lambda: signal(lane_sem.at[1, d], jnp.maximum(me - group, 0)))

        @pl.when(has_down)
        def _():
            pl.semaphore_wait(lane_sem.at[0, d], 1)

        @pl.when(has_up)
        def _():
            pl.semaphore_wait(lane_sem.at[1, d], 1)

    column[...] = jnp.zeros_like(column)

    sums = jnp.zeros((half, LANE), jnp.float32)
    dates = lax.broadcasted_iota(jnp.int32, (half, LANE), 0)
    for part in range(2):
        load(part).wait()
        chunk = slice(part * part_rows, (part + 1) * part_rows)
        wide[chunk, :] = raw[chunk, :].astype(jnp.float32)
        for q in range(rows):
            for block in range(blocks):
                start = part * part_rows + block * rows + place(q)
                piece = wide[pl.ds(start, half, stride=stride), :]
                piece = jnp.where(dates < ndate, piece, 0.0)
                scene[HALF + q, block, part * half:(part + 1) * half, :] = piece.astype(jnp.bfloat16)
                sums = sums + piece * piece
    column[0:half, :] = sums
    powers[lane] = jnp.sum(column[0:long_dates, :].T, axis=0, keepdims=True)

    load_index.wait()
    target = index_ref[0]
    target_row = lax.div(target, cols) - first_row
    target_col = lax.rem(target, cols)
    base = jnp.clip(lax.div(target_col + SUB - HALF, SUB) - 1, 0, cols // SUB - 2)
    home = lax.broadcasted_iota(jnp.int32, (1, long_depth), 1) * 0 + target_row

    def turn(slot):
        for block in range(blocks):
            lines = slice(block * LANE, (block + 1) * LANE)
            for i in range(tiles):
                deep = slice(i * LANE, min((i + 1) * LANE, depth))
                tile = scene[slot, block, deep, :]
                if tile.shape[0] < LANE:
                    tile = jnp.concatenate([tile, jnp.zeros((LANE - tile.shape[0], LANE), tile.dtype)], axis=0)
                turned[slot, i, lines, :] = tile.T

    def pick(slot):
        group_of = lax.broadcasted_iota(jnp.int32, (SUB, LANE), 1) * 0 + base
        hits = [(group_of == k).astype(jnp.float32).astype(scene.dtype) for k in range(-1, cols // SUB)]
        strips = []
        for i in range(tiles):
            first = jnp.zeros((SUB, LANE), scene.dtype)
            second = first
            for k in range(cols // SUB):
                piece = turned[slot, i, k * SUB:(k + 1) * SUB, :]
                first = first + piece * hits[k + 1]
                second = second + piece * hits[k]
            strips.append(jnp.concatenate([first, second], axis=0))
        shape = (SUB, 2 * SUB)
        offset = lax.broadcasted_iota(jnp.int32, shape, 0)
        line = lax.broadcasted_iota(jnp.int32, shape, 1)
        hit = (line == target_col - HALF - base * SUB + offset) & (offset < WIDTH)
        left = hit.astype(jnp.float32).astype(scene.dtype)
        found = jnp.dot(left, jnp.concatenate(strips, axis=1), preferred_element_type=jnp.float32)
        picks[slot] = found[0:EIGHT].astype(scene.dtype)

    pl.semaphore_wait(barrier, expected)
    if planes > 1:
        pl.when(outer)(lambda: signal(meet_sem, near))

    def mate_copy(k, rows_sent):
        return pltpu.make_async_remote_copy(
            src_ref=powers.at[rows_sent], dst_ref=powers.at[rows_sent],
            send_sem=power_sem.at[0], recv_sem=power_sem.at[1],
            device_id={"row": plane * group + lax.rem(lane + k, group)}, device_id_type=MESH,
        )

    def plane_copy(k, rows_sent, aside):
        target = lax.rem(plane + k, planes) * group + lane
        return pltpu.make_async_remote_copy(
            src_ref=plane_rows.at[rows_sent], dst_ref=plane_rows.at[rows_sent],
            send_sem=plane_sem.at[aside], recv_sem=plane_sem.at[2],
            device_id={"row": target + aside * (near - me)}, device_id_type=MESH,
        )

    def ref_copy(k, rows_sent):
        return pltpu.make_async_remote_copy(
            src_ref=refs.at[rows_sent], dst_ref=refs.at[rows_sent],
            send_sem=ref_sem.at[0], recv_sem=ref_sem.at[1],
            device_id={"row": peer(k)}, device_id_type=MESH,
        )

    mate_all = mate_copy(1, pl.ds(0, group - 1))
    ref_all = ref_copy(1, pl.ds(0, n - 1))
    if planes > 1:
        plane_all = [plane_copy(1, pl.ds(0, planes - 1), aside) for aside in range(2)]


    far_id = jnp.clip(far, 0, n - 1)
    near_id = jnp.clip(near, 0, n - 1)

    def far_copy(t, chunk=slice(None), deep=slice(None)):
        return pltpu.make_async_remote_copy(
            src_ref=scene.at[HALF + t, chunk, deep], dst_ref=scene.at[HALF - 1 - t, chunk, deep],
            send_sem=far_sem.at[HALF], recv_sem=far_sem.at[t],
            device_id={"row": far_id}, device_id_type=MESH,
        )

    far_first = far_copy(0, pl.ds(0, 1), pl.ds(0, half))

    def near_copy(t):
        return pltpu.make_async_remote_copy(
            src_ref=scene.at[HALF + rows - 1 - t], dst_ref=scene.at[HALF + rows + t],
            send_sem=near_sem.at[0], recv_sem=near_sem.at[1],
            device_id={"row": near_id}, device_id_type=MESH,
        )

    near_all = pltpu.make_async_remote_copy(
        src_ref=scene.at[pl.ds(HALF + rows - HALF, HALF)], dst_ref=scene.at[pl.ds(HALF + rows, HALF)],
        send_sem=near_sem.at[0], recv_sem=near_sem.at[1],
        device_id={"row": near_id}, device_id_type=MESH,
    )
    far_all = pltpu.make_async_remote_copy(
        src_ref=scene.at[pl.ds(HALF, HALF)], dst_ref=scene.at[pl.ds(0, HALF)],
        send_sem=far_sem.at[HALF], recv_sem=far_sem.at[0],
        device_id={"row": far_id}, device_id_type=MESH,
    )
    piece_copy = pltpu.make_async_remote_copy(
        src_ref=pieces, dst_ref=picks.at[pl.ds(0, HALF)],
        send_sem=piece_sem.at[0], recv_sem=piece_sem.at[1],
        device_id={"row": far_id}, device_id_type=MESH,
    )

    def send_rest():
        piece_copy.start()
        far_copy(0, pl.ds(0, 1), pl.ds(half, half)).start()
        far_copy(0, pl.ds(1, blocks - 1)).start()
        for t in range(1, HALF):
            far_copy(t).start()

    for k in range(1, group):
        mate_copy(k, lane).start()
    pl.when(inner & has_far)(far_first.start)
    for q in range(rows):
        turn(HALF + q)
        pick(HALF + q)
    for t in range(HALF):
        pieces[HALF - 1 - t] = picks[HALF + t]
    pl.when(inner & has_far)(send_rest)

    @pl.when(jnp.logical_not(has_far))
    def _():
        scene[0:HALF] = jnp.zeros((HALF, blocks, depth, LANE), scene.dtype)
        picks[0:HALF] = jnp.zeros((HALF, EIGHT, long_depth), scene.dtype)

    @pl.when(jnp.logical_not(has_near))
    def _():
        scene[HALF + rows:span] = jnp.zeros((HALF, blocks, depth, LANE), scene.dtype)

    load_mask.wait()
    row_ids = first_row + lax.broadcasted_iota(jnp.int32, (rows, cols), 0)
    col_ids = lax.broadcasted_iota(jnp.int32, (rows, cols), 1)
    count = jnp.zeros((rows, cols), jnp.float32)
    ones = []
    for a in range(WIDTH):
        step = a + odd * (WIDTH - 1 - 2 * a)
        for b in range(WIDTH):
            there = row_ids + (step - HALF)
            inside = (there >= 0) & (there < total_rows)
            inside = inside & (col_ids + (b - HALF) >= 0) & (col_ids + (b - HALF) < cols)
            if (a, b) != (HALF, HALF):
                inside = inside & (mask_ref[step * WIDTH + b] == 1)
            one = inside.astype(jnp.float32)
            ones.append(one)
            count = count + one
    inverse = 1.0 / (count * ndate)
    chosen[...] = jnp.zeros_like(chosen)
    for o in range(WIDTH * WIDTH):
        line = ones[o] * inverse
        for q in range(rows):
            spot = o // WIDTH * EIGHT + o % WIDTH
            chosen[q, spot:spot + 1, :] = jnp.where(odd == 1, line[rows - 1 - q:rows - q], line[q:q + 1])

    def window(block):
        return max(0, block * LANE - SUB), min(cols, (block + 1) * LANE + SUB)

    coef[...] = jnp.zeros_like(coef)
    late[...] = jnp.zeros_like(late)
    for block in range(blocks):
        begin, end = window(block)
        shape = (end - begin, LANE)
        shift = begin - block * LANE
        shift = shift + lax.broadcasted_iota(jnp.int32, shape, 0) - lax.broadcasted_iota(jnp.int32, shape, 1)
        for q in range(rows):
            for a in range(WIDTH):
                band = jnp.zeros(shape, jnp.float32)
                for b in range(WIDTH):
                    line = chosen[q, a * EIGHT + b:a * EIGHT + b + 1, block * LANE:(block + 1) * LANE]
                    band = jnp.where(shift == b - HALF, line, band)
                weight[block, q, a, 0:end - begin, :] = band

    def sides(block):
        ends = []
        if block > 0:
            ends.append(block * LANE - SUB)
        if block < blocks - 1:
            ends.append((block + 1) * LANE)
        return ends

    def set_edges(low):
        for block in range(blocks):
            for i in range(tiles):
                parts = []
                for end in sides(block):
                    if low > 0:
                        parts.append(jnp.zeros((low * SUB, LANE), edges.dtype))
                    for slot in range(low, span):
                        parts.append(turned[slot, i, end:end + SUB, :])
                used = len(sides(block)) * span * SUB
                if used < edges.shape[2]:
                    parts.append(jnp.zeros((edges.shape[2] - used, LANE), edges.dtype))
                edges[block, i * LANE:(i + 1) * LANE, :] = jnp.concatenate(parts, axis=0).T

    for t in range(HALF):
        pl.when(has_near)(near_copy(t).start)
    mate_all.wait_recv()
    if planes > 1:
        @pl.when(outer & has_far)
        def _():
            far_first.start()
            send_rest()
    plane_rows[plane] = jnp.sum(powers[...], axis=0)
    if planes > 1:
        @pl.when(inner)
        def _():
            pl.semaphore_wait(meet_sem, 1)
            for d in range(planes - 2):
                meet_lane(d)
            for k in range(1, planes):
                for aside in range(2):
                    plane_copy(k, plane, aside).start()

        plane_all[0].wait_recv()
    power = jnp.sum(plane_rows[...], axis=0)
    gain_row = lax.rsqrt(power * (1.0 / (total_rows * cols)) + 0.1)
    gains[...] = jnp.broadcast_to(gain_row, (LANE, long_dates)).T[0:half, :]
    tall = jnp.concatenate([gains[...], gains[...], jnp.zeros((long_depth - depth, LANE), jnp.float32)], axis=0)
    long_gain[...] = tall.T[0:8, :]

    def set_pair(q, block, real, imag):
        pairs[q, block, 0, 0:half, :] = real
        pairs[q, block, 1, 0:half, :] = imag
        pairs[q, block, 0, half:depth, :] = imag
        pairs[q, block, 1, half:depth, :] = -real

    for q in range(rows):
        for block in range(blocks):
            square = gains[...] * gains[...]
            tile = scene[HALF + q, block].astype(jnp.float32)
            set_pair(
                q, block, (tile[0:half] * square).astype(jnp.bfloat16), (tile[half:depth] * square).astype(jnp.bfloat16)
            )

    def project(q, block, slots, into_late=False, factor=None):
        begin, end = window(block)
        size = end - begin
        main = block * LANE - begin
        left = jnp.concatenate(
            [jnp.concatenate([turned[slot, i, begin:end, :] for i in range(tiles)], axis=1) for slot in slots], axis=0
        )
        right = jnp.concatenate([pairs[q, block, 0], pairs[q, block, 1]], axis=1)
        proj = jnp.dot(left[:, 0:depth], right, preferred_element_type=jnp.float32)
        for i, slot in enumerate(slots):
            a = slot - q
            band = weight[block, q, a, 0:size, :]
            if factor is not None:
                band = band * factor
            for c in range(2):
                part = (proj[i * size:(i + 1) * size, c * LANE:(c + 1) * LANE] * band).astype(jnp.bfloat16)
                if into_late:
                    late[q, block, c, begin:end, :] = part
                    continue
                coef[q, block, c, a * LANE:(a + 1) * LANE, :] = part[main:main + LANE]
                for k, side in enumerate(sides(block)):
                    spot = WIDTH * LANE + (k * span + slot) * SUB
                    coef[q, block, c, spot:spot + SUB, :] = part[side - begin:side - begin + SUB]

    def update(q, block, slots):
        left = jnp.concatenate([scene[s, block] for s in slots] + [edges[block, 0:depth, :]], axis=1)
        first = (slots[0] - q) * LANE
        right = jnp.concatenate([coef[q, block, 0, first:, :], coef[q, block, 1, first:, :]], axis=1)
        return jnp.dot(left, right, preferred_element_type=jnp.float32)

    def late_update(q, block, slot):
        left = jnp.concatenate([scene[slot, b] for b in range(blocks)], axis=1)
        right = jnp.concatenate([late[q, block, 0], late[q, block, 1]], axis=1)
        return jnp.dot(left, right, preferred_element_type=jnp.float32)

    def combine(product):
        gain = gains[...]
        top, bottom = product[0:half], product[half:depth]
        real = (top[:, 0:LANE] - bottom[:, LANE:2 * LANE]) * gain
        imag = (top[:, LANE:2 * LANE] + bottom[:, 0:LANE]) * gain
        energy = jnp.sum(real * real + imag * imag, axis=0, keepdims=True)
        return real, imag, lax.rsqrt(energy * (1.0 / ndate) + 0.001)

    def first_step(q, block, product):
        real, imag, factor = combine(product)
        gain = gains[...]
        set_pair(q, block, (real * gain).astype(jnp.bfloat16), (imag * gain).astype(jnp.bfloat16))
        return factor

    def last_steps(q, factors):
        window_slots = list(range(q, q + WIDTH))
        for i in range(1, ITERS):
            for block in range(blocks):
                project(q, block, window_slots, factor=factors[block])
            products = [update(q, block, window_slots) for block in range(blocks)]
            if i < ITERS - 1:
                factors = [first_step(q, block, products[block]) for block in range(blocks)]
        for block in range(blocks):
            real, imag, factor = combine(products[block])
            vectors[place(q), block, 0:half, :] = real * factor
            vectors[place(q), block, half:depth, :] = imag * factor

    def seen(q, slots):
        return [s for s in slots if q <= s < q + WIDTH]

    pl.when(has_near)(near_all.wait_recv)
    pl.when(has_far)(piece_copy.wait_recv)
    for t in range(HALF):
        turn(HALF + rows + t)
        pick(HALF + rows + t)
    set_edges(HALF)
    for q in range(rows):
        slots = seen(q, range(HALF, span))
        for block in range(blocks):
            project(q, block, slots)
        for block in range(blocks):
            total[q, block] = update(q, block, slots)

    def swap(x):
        lanes = lax.broadcasted_iota(jnp.int32, x.shape, 1)
        ahead = pltpu.roll(x, long_depth - half, 1)
        behind = pltpu.roll(x, half, 1)
        return jnp.where(lanes < half, -ahead, jnp.where(lanes < depth, behind, 0.0))

    def reference_vector(q):
        stack = jnp.concatenate([picks[q + a].astype(jnp.float32) for a in range(WIDTH)], axis=0)
        lanes = lax.broadcasted_iota(jnp.int32, (WIDTH * EIGHT, cols), 1)
        bands = jnp.sum(jnp.where(lanes == target_col, chosen[q], 0.0), axis=1, keepdims=True)
        middle = HALF * EIGHT + HALF
        center = stack[middle:middle + 1]
        gain = long_gain[0:1, :]
        vector = center * gain
        for _ in range(ITERS):
            vector = vector * gain
            proj_real = jnp.sum(stack * vector, axis=1, keepdims=True) * bands
            proj_imag = jnp.sum(stack * -swap(vector), axis=1, keepdims=True) * bands
            vector = jnp.sum(stack * proj_real, axis=0, keepdims=True)
            vector = vector + swap(jnp.sum(stack * proj_imag, axis=0, keepdims=True))
            vector = vector * gain
            energy = jnp.sum(vector * vector, axis=1, keepdims=True)
            vector = vector * lax.rsqrt(energy * (1.0 / ndate) + 0.001)
        return vector

    found = jnp.zeros((1, long_depth), jnp.float32)
    for q in range(rows):
        found = found + jnp.where(home == place(q), reference_vector(q), 0.0)
    refs[me] = found
    for k in range(1, n):
        ref_copy(k, me).start()

    for q in range(HALF, rows):
        last_steps(q, [first_step(q, block, total[q, block]) for block in range(blocks)])
    for t in range(HALF):
        slot = HALF - 1 - t
        pl.when(has_far)(far_copy(t).wait_recv)
        turn(slot)
        set_edges(slot)
        for q in range(min(slot, rows - 1), -1, -1):
            for block in range(blocks):
                project(q, block, [slot], into_late=True)
        if slot < rows:
            products = [late_update(slot, block, slot) for block in range(blocks)]
            factors = [first_step(slot, block, total[slot, block] + products[block]) for block in range(blocks)]
            last_steps(slot, factors)
        for q in range(min(slot, rows) - 1, -1, -1):
            for block in range(blocks):
                total[q, block] += late_update(q, block, slot)

    ref_all.wait_recv()
    refvec = jnp.sum(refs[...], axis=0)
    columns[...] = jnp.broadcast_to(refvec, (LANE, long_depth)).T[0:depth]

    pl.when(has_far)(far_all.wait_send)
    pl.when(has_far)(piece_copy.wait_send)
    pl.when(has_near)(near_all.wait_send)
    mate_all.wait_send()
    ref_all.wait_send()
    if planes > 1:
        @pl.when(inner)
        def _():
            plane_all[0].wait_send()
            plane_all[1].wait_send()


def per_device(slc, mask, ref_index):
    parts, ndate, rows, cols = slc.shape
    n = lax.axis_size("row")
    group = GROUP if n % GROUP == 0 else n
    half = round_up(ndate, SUB)
    depth = 2 * half
    long_dates = round_up(half, LANE)
    long_depth = round_up(depth, LANE)
    blocks = cols // LANE
    span = rows + 2 * HALF
    lines = parts * ndate * blocks * rows
    margin = round_up(min(2, blocks - 1) * span * SUB, LANE)
    x = slc.reshape(parts, ndate, rows, blocks, LANE).transpose(0, 1, 3, 2, 4).reshape(lines, LANE)
    vmem = pl.BlockSpec(memory_space=pltpu.VMEM)
    anywhere = pl.BlockSpec(memory_space=pltpu.HBM)

    def body(*refs):
        kernel(n, ndate, *refs)

    def in_hbm(array):
        return pltpu.with_memory_space_constraint(array, pltpu.HBM)

    vectors, columns = pl.pallas_call(
        body,
        out_shape=(
            jax.ShapeDtypeStruct((rows, blocks, depth, LANE), jnp.float32),
            jax.ShapeDtypeStruct((depth, LANE), jnp.float32),
        ),
        in_specs=[anywhere, anywhere, anywhere],
        out_specs=(vmem, vmem),
        scratch_shapes=[
            pltpu.VMEM((lines, LANE), jnp.bfloat16),
            pltpu.VMEM(mask.shape, jnp.int32),
            pltpu.SMEM(ref_index.shape, jnp.int32),
            pltpu.VMEM((lines + (half - ndate) * blocks * rows, LANE), jnp.float32),
            pltpu.VMEM((span, blocks, depth, LANE), jnp.bfloat16),
            pltpu.VMEM((span, long_depth // LANE, cols, LANE), jnp.bfloat16),
            pltpu.VMEM((rows, WIDTH * EIGHT, cols), jnp.float32),
            pltpu.VMEM((span, EIGHT, long_depth), jnp.bfloat16),
            pltpu.VMEM((HALF, EIGHT, long_depth), jnp.bfloat16),
            pltpu.VMEM((blocks, rows, WIDTH, LANE + 2 * SUB, LANE), jnp.float32),
            pltpu.VMEM((rows, blocks, 2, depth, LANE), jnp.bfloat16),
            pltpu.VMEM((rows, blocks, 2, WIDTH * LANE + margin, LANE), jnp.bfloat16),
            pltpu.VMEM((rows, blocks, 2, cols, LANE), jnp.bfloat16),
            pltpu.VMEM((blocks, long_depth, margin), jnp.bfloat16),
            pltpu.VMEM((rows, blocks, depth, 2 * LANE), jnp.float32),
            pltpu.VMEM((half, LANE), jnp.float32),
            pltpu.VMEM((8, long_depth), jnp.float32),
            pltpu.VMEM((long_depth, LANE), jnp.float32),
            pltpu.VMEM((group, 1, long_dates), jnp.float32),
            pltpu.VMEM((n // group, 1, long_dates), jnp.float32),
            pltpu.VMEM((n, 1, long_depth), jnp.float32),
            pltpu.SemaphoreType.DMA((2,)),
            pltpu.SemaphoreType.DMA,
            pltpu.SemaphoreType.DMA,
            pltpu.SemaphoreType.REGULAR,
            pltpu.SemaphoreType.REGULAR((2, max(1, n // group - 2))),
            pltpu.SemaphoreType.DMA((HALF + 1,)),
            pltpu.SemaphoreType.DMA((2,)),
            pltpu.SemaphoreType.DMA((2,)),
            pltpu.SemaphoreType.DMA((2,)),
            pltpu.SemaphoreType.DMA((3,)),
            pltpu.SemaphoreType.DMA((2,)),
        ],
        compiler_params=pltpu.CompilerParams(collective_id=0, has_side_effects=True, vmem_limit_bytes=VMEM_LIMIT),
        name="link",
    )(in_hbm(x), in_hbm(mask), ref_index)

    def put(vectors, columns, out_ref, stage, sem):
        size = round_up(ndate // PUTS, EIGHT)
        copies = []
        for k in range(PUTS):
            first, last = k * size, min((k + 1) * size, ndate)
            low, high = slice(first, last), slice(half + first, half + last)
            ref_real, ref_imag = columns[low, :], columns[high, :]
            for block in range(blocks):
                for row in range(rows):
                    real, imag = vectors[row, block, low, :], vectors[row, block, high, :]
                    start = (first * blocks + block) * rows + row
                    stride = blocks * rows
                    stage[pl.ds(start, last - first, stride=stride), :] = real * ref_real + imag * ref_imag
                    start = start + ndate * stride
                    stage[pl.ds(start, last - first, stride=stride), :] = imag * ref_real - real * ref_imag
            for part in range(parts):
                chunk = pl.ds((part * ndate + first) * blocks * rows, (last - first) * blocks * rows)
                copy = pltpu.make_async_copy(stage.at[chunk], out_ref.at[chunk], sem.at[k, part])
                copy.start()
                copies.append(copy)
        for copy in copies:
            copy.wait()

    out = pl.pallas_call(
        put,
        out_shape=jax.ShapeDtypeStruct((lines, LANE), jnp.float32),
        in_specs=[vmem, vmem],
        out_specs=anywhere,
        scratch_shapes=[pltpu.VMEM((lines, LANE), jnp.float32), pltpu.SemaphoreType.DMA((PUTS, parts))],
        compiler_params=pltpu.CompilerParams(vmem_limit_bytes=16 * 1024 * 1024),
        name="put",
    )(vectors, columns)
    out = out.reshape(parts, ndate, blocks, rows, LANE).transpose(0, 1, 3, 2, 4)
    return out.reshape(parts, ndate, rows, cols)


def solution(mesh):
    placed = (P(None, None, ("grp", "row"), None), P(None, ("grp", "row"), None), P("grp"))
    return jax.shard_map(
        per_device,
        mesh=mesh,
        in_specs=placed,
        out_specs=P(None, None, ("grp", "row"), None),
        check_vma=False,
    )
```
